512 devices in a mesh: fft: 64 (over y, z), grp: 8 (over x, core).
Axes of the slice: x: 4, y: 4, z: 16, core: 2. Of those that a mesh axis runs over, the one named last changes fastest.
Arguments:
- potential: float32 [4, 256, 256, 256], P(None, 'fft', 'grp'), may hold values from -6 to 6
- stick_mill: int32 [2, 1024], replicated, may hold values from -128 to 127, as said below
- positions: int32 [3, 1024], P(None, 'grp'), may hold values from 0 to 255
- aug_charge: bfloat16 [171, 1024, 256], P(None, 'fft'), may hold values from -0.01171875 to 0.01171875
Outputs:
- vg_sticks: float32 [4, 2, 1024, 256], P(None, None, 'fft')
- d_matrix: float32 [4, 171, 1024], P(None, None, 'grp')
The draws below stay inside these ranges and needn't reach their ends.
Inputs may be any that keep to these rules, and one draw needn't show every extreme that they name: `stick_mill`: stick k is owned by fft index k // 16; no two sticks have the same (gx, gy), and every stick has gx^2 + gy^2 < 128^2.
All inputs are finite; a program needn't handle non-finite values.
Results may differ from the reference program's by a relative error of at most 0.0029.
Values sent between devices are 32-bit elements; how exact they have to be, the bound alone decides.
No kernel may reach another device: no remote copies, remote signals or barrier semaphores. Data moves between devices by JAX's collectives and lax.ppermute only.
A program may use at most 128 MiB of HBM per device.

```python
import math
import jax
import jax.numpy as jnp
from jax import lax

N = 256
SPINS = 4
PAIRS = 171
ATM_GRP = 128
STICKS = 1024
ATOMS = 1024
N_GRP = 8


def draw_stick_mill(key, part):
    shuffled = jax.random.permutation(jax.random.fold_in(key, 7), N * N).astype(jnp.int32)
    col_gx = shuffled // N - N // 2
    col_gy = jnp.mod(shuffled, N) - N // 2
    outside = (col_gx * col_gx + col_gy * col_gy >= N // 2 * (N // 2)).astype(jnp.int32)
    priority = jnp.arange(N * N, dtype=jnp.int32) + outside * (N * N)
    ranking = jnp.argsort(priority, stable=True)[:STICKS]
    chosen = shuffled[ranking]
    return jnp.stack([chosen // N - N // 2, jnp.mod(chosen, N) - N // 2]).astype(jnp.int32)


def with_ends(array, key, low, high):
    longest = array.shape.index(max(array.shape))
    spots = []
    for shift in (0, 1):
        where = [jax.random.randint(jax.random.fold_in(key, axis), (), 0, length) for axis, length in enumerate(array.shape)]
        where[longest] = (where[longest] + shift) % array.shape[longest]
        spots.append(tuple(where))
    return array.at[spots[0]].set(low).at[spots[1]].set(high)


def level_of(key, shape, shards, least, top_value):
    gain = 1.0
    for dim, blocks in shards:
        heights = jax.random.uniform(jax.random.fold_in(jax.random.fold_in(key, 6), dim), (blocks,), jnp.float32, least / len(shards), top_value / len(shards))
        gain = gain * jnp.repeat(jnp.exp(heights), shape[dim] // blocks).reshape((-1,) + (1,) * (len(shape) - 1 - dim))
    return gain


def normal_values(rng, dims, scale, most, split=(), kind=jnp.bfloat16):
    gain = level_of(rng, dims, split, -0.22, 0.18) if split else 1.0
    values = jax.random.normal(rng, dims, jnp.float32) * scale * gain
    return jnp.minimum(jnp.maximum(values, -most), most).astype(kind)


def setup_inputs(seed: int = 0) -> dict:
    key_of = jax.random.split(jax.random.key(seed), 5)
    return {
        "potential": normal_values(key_of[0], (SPINS, N, N, N), 1.0, 6.0, ((1, 64), (2, 8)), jnp.float32),
        "stick_mill": draw_stick_mill(jax.random.fold_in(key_of[4], 71), 0),
        "positions": with_ends(jax.random.randint(key_of[2], (3, ATOMS), 0, N), jax.random.fold_in(key_of[2], 1), 0, N - 1).astype(jnp.int32),
        "aug_charge": normal_values(key_of[3], (PAIRS, STICKS, N), (STICKS * N) ** -0.5, 0.01171875, ((1, 64),)),
    }


two_pi = 2.0 * math.pi


def reference(potential, stick_mill, positions, aug_charge):
    norm_factor = float(N) ** -1.5
    spectrum = jnp.fft.fftn(potential, axes=(1, 2, 3))
    grid_index = jnp.arange(N, dtype=jnp.int32)
    shifted = grid_index - N // 2
    plane_index = jnp.mod(shifted, N)
    row_index = jnp.mod(stick_mill[1], N)
    col_index = jnp.mod(stick_mill[0], N)
    picked = spectrum[:, plane_index[None, :], row_index[:, None], col_index[:, None]]
    vg_sticks = (jnp.stack([jnp.real(picked), jnp.imag(picked)], axis=1) * norm_factor).astype(jnp.float32)
    charge = aug_charge.astype(jnp.float32).reshape(PAIRS, STICKS * N)
    pos_blocks = positions.reshape(3, N_GRP, ATM_GRP).transpose(1, 0, 2)

    def atom_block(pos_group):
        phase_k = jnp.mod(stick_mill[0][:, None, None] * pos_group[0][None, None, :]
                          + stick_mill[1][:, None, None] * pos_group[1][None, None, :]
                          + shifted[None, :, None] * pos_group[2][None, None, :], N)
        angle_all = (two_pi / N) * phase_k.astype(jnp.float32)
        cosine = jnp.cos(angle_all)
        sine = jnp.sin(angle_all)
        results = []
        for channel in range(SPINS):
            mixed_term = vg_sticks[channel, 0][:, :, None] * cosine - vg_sticks[channel, 1][:, :, None] * sine
            rounded = lax.optimization_barrier(mixed_term.astype(jnp.bfloat16)).astype(jnp.float32)
            results.append(jnp.dot(charge, rounded.reshape(STICKS * N, ATM_GRP),
                                   precision=lax.Precision.HIGHEST, preferred_element_type=jnp.float32))
        return jnp.stack(results)

    blocks_out = lax.map(atom_block, pos_blocks)
    d_matrix = blocks_out.transpose(1, 2, 0, 3).reshape(SPINS, PAIRS, ATOMS)
    return vg_sticks, d_matrix
```

```python
import functools
import math

import jax
import jax.numpy as jnp
import numpy as np
from jax import lax
from jax.experimental import pallas as pl
from jax.experimental.pallas import tpu as pltpu
from jax.sharding import Mesh
from jax.sharding import PartitionSpec as P

N = 256
ROWS = ("y", "x", "core")
GRP = ("x", "core")
FFT = ("y", "z")
F32 = jnp.float32
BF16 = jnp.bfloat16


def split_table(table):
    high = table.astype(np.float32).astype(jnp.bfloat16)
    low = (table - high.astype(np.float64)).astype(np.float32).astype(jnp.bfloat16)
    return high, low


def wave_table(left, right):
    angle = 2.0 * math.pi / N * np.mod(np.outer(left, right), N)
    return np.concatenate([np.cos(angle), np.sin(angle)], axis=1)


def split_value(x):
    high = x.astype(BF16)
    return high, (x - high.astype(F32)).astype(BF16)


def dot(a, b):
    return jnp.dot(a, b, preferred_element_type=F32)


def plane_kernel(grp_ref, pot_ref, mill_ref, hi_ref, lo_ref, out_ref, stack, turned):
    cols = jnp.bitwise_and(mill_ref[...], N - 1)
    grid = lax.broadcasted_iota(jnp.int32, (N, 1024), 0)
    pick_x = jnp.where(grid == cols[0:1, :], 1.0, 0.0).astype(BF16)
    pick_y = jnp.where(grid == cols[1:2, :], 1.0, 0.0).astype(BF16)
    start = pl.multiple_of(grp_ref[0] * 32, 32)
    near_hi = hi_ref[pl.ds(start, 32), :]
    near_lo = lo_ref[pl.ds(start, 32), :]
    cos_y = dot(near_hi[:, :N], pick_y) + dot(near_lo[:, :N], pick_y)
    sin_y = dot(near_hi[:, N:], pick_y) + dot(near_lo[:, N:], pick_y)
    hi = hi_ref[...]
    lo = lo_ref[...]
    for c in range(4):
        p_hi, p_lo = split_value(pot_ref[c * 128 : (c + 1) * 128, :])
        wave = dot(p_hi, hi) + dot(p_hi, lo) + dot(p_lo, hi)
        w_hi, w_lo = split_value(wave)
        even = dot(w_hi[:, :N], pick_x) + dot(w_lo[:, :N], pick_x)
        odd = dot(w_hi[:, N:], pick_x) + dot(w_lo[:, N:], pick_x)
        for z in range(4):
            e = even[z * 32 : (z + 1) * 32, :]
            o = odd[z * 32 : (z + 1) * 32, :]
            real = jnp.sum(e * cos_y - o * sin_y, axis=0, keepdims=True)
            imag = -jnp.sum(e * sin_y + o * cos_y, axis=0, keepdims=True)
            for z0 in range(2):
                for j in range(2):
                    row = z0 * 64 + z * 16 + j * 4 + c
                    stack[row : row + 1, :] = real
                    stack[row + 8 : row + 9, :] = imag
    for b in range(8):
        turned[b * 128 : (b + 1) * 128, :] = stack[:, b * 128 : (b + 1) * 128].T
    lane = lax.broadcasted_iota(jnp.int32, (8, 128), 1)
    upper = lane >= 64
    second = jnp.bitwise_and(lane, 4) != 0
    for y in range(4):
        for g in range(8):
            base = y * 256 + g * 2
            parts = [turned[pl.ds(base + z0 * 16 + j, 8, 32), :] for z0 in range(2) for j in range(2)]
            tile = jnp.where(upper, jnp.where(second, parts[3], parts[2]), jnp.where(second, parts[1], parts[0]))
            at = (y * 8 + g) * 8
            out_ref[at : at + 8, :] = tile


def plane_part(potential, stick_mill, grp, hi, lo):
    return pl.pallas_call(
        plane_kernel,
        out_shape=jax.ShapeDtypeStruct((256, 128), F32),
        in_specs=[pl.BlockSpec(memory_space=pltpu.SMEM)] + [pl.BlockSpec(memory_space=pltpu.VMEM)] * 4,
        out_specs=pl.BlockSpec(memory_space=pltpu.VMEM),
        scratch_shapes=[pltpu.VMEM((128, 1024), F32), pltpu.VMEM((1024, 128), F32)],
        name="plane_part",
    )(grp, potential, stick_mill, hi, lo)


def fold_kernel(in_ref, out_ref):
    lane = lax.broadcasted_iota(jnp.int32, (8, 128), 1)
    lower = lane < 64
    sums = []
    for y in range(4):
        total = in_ref[y * 64 : y * 64 + 8, :]
        for g in range(1, 8):
            total = total + in_ref[y * 64 + g * 8 : y * 64 + g * 8 + 8, :]
        sums.append(total)
    for yp in range(2):
        a, b = sums[2 * yp], sums[2 * yp + 1]
        out_ref[pl.ds(yp, 8, 4), :] = jnp.where(lower, a, pltpu.roll(b, 64, 1))
        out_ref[pl.ds(2 + yp, 8, 4), :] = jnp.where(lower, pltpu.roll(a, 64, 1), b)


def folded(arrived):
    return pl.pallas_call(
        fold_kernel,
        out_shape=jax.ShapeDtypeStruct((32, 128), F32),
        in_specs=[pl.BlockSpec(memory_space=pltpu.VMEM)],
        out_specs=pl.BlockSpec(memory_space=pltpu.VMEM),
        name="fold",
    )(arrived)


def line_kernel(in_ref, hi_ref, lo_ref, out_ref):
    x = in_ref[...]
    t = jnp.concatenate([x, x, x, x], axis=0).T
    lane = lax.broadcasted_iota(jnp.int32, (16, 128), 1)
    halves = []
    for y0 in range(2):
        tile = t[y0 * 64 : y0 * 64 + 16, :]
        for z in range(1, 4):
            at = y0 * 64 + z * 16
            tile = jnp.where(lane >= 32 * z, t[at : at + 16, :], tile)
        halves.append(tile)
    a = jnp.concatenate(halves, axis=1)
    a_hi, a_lo = split_value(a)
    hi = hi_ref[...]
    r = dot(a_hi, hi) + dot(a_hi, lo_ref[...]) + dot(a_lo, hi)
    real = r[0:8, :N] + r[8:16, N:]
    imag = r[8:16, :N] - r[0:8, N:]
    for g in range(8):
        out_ref[g, 0:8, :] = real
        out_ref[g, 8:16, :] = imag


def line_part(arrived, hi, lo):
    return pl.pallas_call(
        line_kernel,
        out_shape=jax.ShapeDtypeStruct((8, 16, N), F32),
        in_specs=[pl.BlockSpec(memory_space=pltpu.VMEM)] * 3,
        out_specs=pl.BlockSpec(memory_space=pltpu.VMEM),
        name="line_part",
    )(arrived, hi, lo)


def phase_kernel(pos_ref, mill_ref, hi_ref, lo_ref, wave_ref, cos_ref, sin_ref):
    zcol = pos_ref[:, 2:3]
    grid = lax.broadcasted_iota(jnp.int32, (128, N), 1)
    pick = jnp.where(grid == zcol, 1.0, 0.0).astype(BF16)
    sign = 1.0 - 2.0 * jnp.bitwise_and(zcol, 1).astype(F32)
    wave_ref[...] = (dot(pick, hi_ref[...]) + dot(pick, lo_ref[...])) * sign
    k = pos_ref[:, 0:1] * mill_ref[0:1, :] + pos_ref[:, 1:2] * mill_ref[1:2, :]
    angle = (2.0 * math.pi / N) * jnp.bitwise_and(k, N - 1).astype(F32)
    cos_ref[...] = jnp.cos(angle)
    sin_ref[...] = jnp.sin(angle)


def phases(pos_cols, mine, hi, lo):
    return pl.pallas_call(
        phase_kernel,
        out_shape=(
            jax.ShapeDtypeStruct((128, 2 * N), F32),
            jax.ShapeDtypeStruct((128, 16), F32),
            jax.ShapeDtypeStruct((128, 16), F32),
        ),
        in_specs=[pl.BlockSpec(memory_space=pltpu.VMEM)] * 4,
        out_specs=(pl.BlockSpec(memory_space=pltpu.VMEM),) * 3,
        name="phases",
    )(pos_cols, mine, hi, lo)


def charge_kernel(v_ref, q_ref, wave_ref, ca_ref, sa_ref, vg_ref, d_ref, mixed):
    for s in range(16):
        g, j = s // 2, s % 2
        ca = ca_ref[:, s : s + 1]
        sa = sa_ref[:, s : s + 1]
        cb = wave_ref[:, :N]
        sb = wave_ref[:, N:]
        cosine = ca * cb - sa * sb
        sine = sa * cb + ca * sb
        for c in range(4):
            row = g * 16 + j * 4 + c
            real = v_ref[row : row + 1, :]
            imag = v_ref[row + 8 : row + 9, :]
            vg_ref[c, 0, s : s + 1, :] = real
            vg_ref[c, 1, s : s + 1, :] = imag
            mixed[c * 128 : (c + 1) * 128, s * N : (s + 1) * N] = (real * cosine - imag * sine).astype(BF16)
    d = lax.dot_general(q_ref[...], mixed[...], (((1,), (1,)), ((), ())), preferred_element_type=F32)
    for c in range(4):
        d_ref[pl.ds(c, 171, 4), :] = d[:, c * 128 : (c + 1) * 128]
    d_ref[684:704, :] = jnp.zeros((20, 128), F32)


def charge_part(v, charge, wave, ca, sa):
    return pl.pallas_call(
        charge_kernel,
        out_shape=(jax.ShapeDtypeStruct((4, 2, 16, N), F32), jax.ShapeDtypeStruct((704, 128), F32)),
        in_specs=[pl.BlockSpec(memory_space=pltpu.VMEM)] * 5,
        out_specs=(pl.BlockSpec(memory_space=pltpu.VMEM),) * 2,
        scratch_shapes=[pltpu.VMEM((512, 4096), BF16)],
        name="charge_part",
    )(v, charge, wave, ca, sa)


def total_kernel(in_ref, out_ref, half):
    total = in_ref[0:88, :]
    for m in range(1, 8):
        total = total + in_ref[m * 88 : (m + 1) * 88, :]
    half[...] = total
    own = half[0:11, :]
    for m in range(1, 8):
        own = own + half[m * 11 : (m + 1) * 11, :]
    for m in range(8):
        half[m * 11 : (m + 1) * 11, :] = own
    full = half[...]
    for m in range(8):
        out_ref[m * 88 : (m + 1) * 88, :] = full


def totals(arrived):
    return pl.pallas_call(
        total_kernel,
        out_shape=jax.ShapeDtypeStruct((704, 128), F32),
        in_specs=[pl.BlockSpec(memory_space=pltpu.VMEM)],
        out_specs=pl.BlockSpec(memory_space=pltpu.VMEM),
        scratch_shapes=[pltpu.VMEM((88, 128), F32)],
        name="totals",
    )(arrived)


def exchange(parts, axes):
    return lax.all_to_all(parts, axes, split_axis=0, concat_axis=0, tiled=True)


def tables():
    index = np.arange(N)
    flat = split_table(wave_table(index, index))
    y0, z4, zs, yp = np.meshgrid(np.arange(2), np.arange(4), np.arange(16), np.arange(2), indexing="ij")
    plane = (((2 * yp + y0) * 16 + zs) * 4 + z4).reshape(-1)
    line = split_table(wave_table(plane, index - N // 2) * float(N) ** -1.5)
    return flat, line


def body(potential, stick_mill, positions, aug_charge):
    (hi, lo), (line_hi, line_lo) = tables()
    hi, lo, line_hi, line_lo = map(jnp.asarray, (hi, lo, line_hi, line_lo))
    grp = lax.axis_index(GRP)
    fft = lax.axis_index(FFT)
    mine = lax.dynamic_slice_in_dim(stick_mill, fft * 16, 16, 1)
    part = plane_part(potential.reshape(512, N), stick_mill, grp.reshape(1), hi, lo)
    arrived = exchange(part.reshape(32, 8, 128), ROWS)
    lines = folded(arrived.reshape(256, 128))
    arrived = exchange(lines.reshape(16, 1, 256), "z")
    copies = line_part(arrived.reshape(32, 128), line_hi, line_lo)
    v = exchange(copies, GRP).reshape(128, N)
    wave, ca, sa = phases(positions.T, mine, hi, lo)
    vg, part = charge_part(v, aug_charge.reshape(171, 16 * N), wave, ca, sa)
    arrived = exchange(part.reshape(64, 1, 1408), FFT)
    own = totals(arrived.reshape(704, 128))
    whole = exchange(own.reshape(64, 1, 1408), FFT)
    return vg, jnp.moveaxis(whole.reshape(176, 4, 128)[:171], 1, 0)


def solution(mesh):
    fine = Mesh(mesh.devices.reshape(4, 16, 4, 2), ("y", "z", "x", "core"))
    placed = (P(None, FFT, GRP, None), P(), P(None, GRP), P(None, FFT, None))
    return jax.shard_map(
        body,
        mesh=fine,
        in_specs=placed,
        out_specs=(P(None, None, FFT, None), P(None, None, GRP)),
        check_vma=False,
    )
```

```python
import functools
import math

import jax
import jax.numpy as jnp
import numpy as np
from jax import lax
from jax.experimental import pallas as pl
from jax.experimental.pallas import tpu as pltpu
from jax.sharding import Mesh
from jax.sharding import PartitionSpec as P

N = 256
ROWS = ("y", "x", "core")
GRP = ("x", "core")
FFT = ("y", "z")
F32 = jnp.float32
BF16 = jnp.bfloat16


def split_table(table):
    high = table.astype(np.float32).astype(jnp.bfloat16)
    low = (table - high.astype(np.float64)).astype(np.float32).astype(jnp.bfloat16)
    return high, low


def wave_table(left, right):
    angle = 2.0 * math.pi / N * np.mod(np.outer(left, right), N)
    return np.concatenate([np.cos(angle), np.sin(angle)], axis=1)


def split_value(x):
    high = x.astype(BF16)
    return high, (x - high.astype(F32)).astype(BF16)


def dot(a, b):
    return jnp.dot(a, b, preferred_element_type=F32)


def plane_kernel(grp_ref, pot_ref, mill_ref, hi_ref, lo_ref, out_ref, stack, turned):
    cols = jnp.bitwise_and(mill_ref[...], N - 1)
    grid = lax.broadcasted_iota(jnp.int32, (N, 1024), 0)
    pick_x = jnp.where(grid == cols[0:1, :], 1.0, 0.0).astype(BF16)
    pick_y = jnp.where(grid == cols[1:2, :], 1.0, 0.0).astype(BF16)
    start = pl.multiple_of(grp_ref[0] * 32, 32)
    near_hi = hi_ref[pl.ds(start, 32), :]
    near_lo = lo_ref[pl.ds(start, 32), :]
    cos_y = dot(near_hi[:, :N], pick_y) + dot(near_lo[:, :N], pick_y)
    sin_y = dot(near_hi[:, N:], pick_y) + dot(near_lo[:, N:], pick_y)
    hi = hi_ref[...]
    lo = lo_ref[...]
    for c in range(4):
        p_hi, p_lo = split_value(pot_ref[c * 128 : (c + 1) * 128, :])
        wave = dot(p_hi, hi) + dot(p_hi, lo) + dot(p_lo, hi)
        w_hi, w_lo = split_value(wave)
        even = dot(w_hi[:, :N], pick_x) + dot(w_lo[:, :N], pick_x)
        odd = dot(w_hi[:, N:], pick_x) + dot(w_lo[:, N:], pick_x)
        for z in range(4):
            e = even[z * 32 : (z + 1) * 32, :]
            o = odd[z * 32 : (z + 1) * 32, :]
            real = jnp.sum(e * cos_y - o * sin_y, axis=0, keepdims=True)
            imag = -jnp.sum(e * sin_y + o * cos_y, axis=0, keepdims=True)
            for z0 in range(2):
                for j in range(2):
                    row = z0 * 64 + z * 16 + j * 4 + c
                    stack[row : row + 1, :] = real
                    stack[row + 8 : row + 9, :] = imag
    for b in range(8):
        turned[b * 128 : (b + 1) * 128, :] = stack[:, b * 128 : (b + 1) * 128].T
    lane = lax.broadcasted_iota(jnp.int32, (8, 128), 1)
    upper = lane >= 64
    second = jnp.bitwise_and(lane, 4) != 0
    for y in range(4):
        for g in range(8):
            base = y * 256 + g * 2
            parts = [turned[pl.ds(base + z0 * 16 + j, 8, 32), :] for z0 in range(2) for j in range(2)]
            tile = jnp.where(upper, jnp.where(second, parts[3], parts[2]), jnp.where(second, parts[1], parts[0]))
            at = (y * 8 + g) * 8
            out_ref[at : at + 8, :] = tile


def plane_part(potential, stick_mill, grp, hi, lo):
    return pl.pallas_call(
        plane_kernel,
        out_shape=pltpu.VMEM((256, 128), F32),
        in_specs=[pl.BlockSpec(memory_space=pltpu.SMEM)] + [pl.BlockSpec(memory_space=pltpu.VMEM)] * 4,
        out_specs=pl.BlockSpec(memory_space=pltpu.VMEM),
        scratch_shapes=[pltpu.VMEM((128, 1024), F32), pltpu.VMEM((1024, 128), F32)],
        name="plane_part",
    )(grp, potential, stick_mill, hi, lo)


def fold_kernel(in_ref, out_ref):
    lane = lax.broadcasted_iota(jnp.int32, (8, 128), 1)
    lower = lane < 64
    sums = []
    for y in range(4):
        total = in_ref[y * 64 : y * 64 + 8, :]
        for g in range(1, 8):
            total = total + in_ref[y * 64 + g * 8 : y * 64 + g * 8 + 8, :]
        sums.append(total)
    for yp in range(2):
        a, b = sums[2 * yp], sums[2 * yp + 1]
        out_ref[pl.ds(yp, 8, 4), :] = jnp.where(lower, a, pltpu.roll(b, 64, 1))
        out_ref[pl.ds(2 + yp, 8, 4), :] = jnp.where(lower, pltpu.roll(a, 64, 1), b)


def folded(arrived):
    return pl.pallas_call(
        fold_kernel,
        out_shape=pltpu.VMEM((32, 128), F32),
        in_specs=[pl.BlockSpec(memory_space=pltpu.VMEM)],
        out_specs=pl.BlockSpec(memory_space=pltpu.VMEM),
        name="fold",
    )(near(arrived))


def line_kernel(in_ref, hi_ref, lo_ref, out_ref):
    x = in_ref[...]
    t = jnp.concatenate([x, x, x, x], axis=0).T
    lane = lax.broadcasted_iota(jnp.int32, (16, 128), 1)
    halves = []
    for y0 in range(2):
        tile = t[y0 * 64 : y0 * 64 + 16, :]
        for z in range(1, 4):
            at = y0 * 64 + z * 16
            tile = jnp.where(lane >= 32 * z, t[at : at + 16, :], tile)
        halves.append(tile)
    a = jnp.concatenate(halves, axis=1)
    a_hi, a_lo = split_value(a)
    hi = hi_ref[...]
    r = dot(a_hi, hi) + dot(a_hi, lo_ref[...]) + dot(a_lo, hi)
    real = r[0:8, :N] + r[8:16, N:]
    imag = r[8:16, :N] - r[0:8, N:]
    for g in range(8):
        out_ref[g, 0:8, :] = real
        out_ref[g, 8:16, :] = imag


def line_part(arrived, hi, lo):
    return pl.pallas_call(
        line_kernel,
        out_shape=pltpu.VMEM((8, 16, N), F32),
        in_specs=[pl.BlockSpec(memory_space=pltpu.VMEM)] * 3,
        out_specs=pl.BlockSpec(memory_space=pltpu.VMEM),
        name="line_part",
    )(near(arrived), hi, lo)


def phase_kernel(pos_ref, mill_ref, hi_ref, lo_ref, wave_ref, cos_ref, sin_ref):
    zcol = pos_ref[:, 2:3]
    grid = lax.broadcasted_iota(jnp.int32, (128, N), 1)
    pick = jnp.where(grid == zcol, 1.0, 0.0).astype(BF16)
    sign = 1.0 - 2.0 * jnp.bitwise_and(zcol, 1).astype(F32)
    wave_ref[...] = (dot(pick, hi_ref[...]) + dot(pick, lo_ref[...])) * sign
    k = pos_ref[:, 0:1] * mill_ref[0:1, :] + pos_ref[:, 1:2] * mill_ref[1:2, :]
    angle = (2.0 * math.pi / N) * jnp.bitwise_and(k, N - 1).astype(F32)
    cos_ref[...] = jnp.cos(angle)
    sin_ref[...] = jnp.sin(angle)


def phases(pos_cols, mine, hi, lo):
    return pl.pallas_call(
        phase_kernel,
        out_shape=(
            pltpu.VMEM((128, 2 * N), F32),
            pltpu.VMEM((128, 16), F32),
            pltpu.VMEM((128, 16), F32),
        ),
        in_specs=[pl.BlockSpec(memory_space=pltpu.VMEM)] * 4,
        out_specs=(pl.BlockSpec(memory_space=pltpu.VMEM),) * 3,
        name="phases",
    )(pos_cols, mine, hi, lo)


def charge_kernel(v_ref, q_ref, wave_ref, ca_ref, sa_ref, vg_ref, d_ref, mixed):
    for s in range(16):
        g, j = s // 2, s % 2
        ca = ca_ref[:, s : s + 1]
        sa = sa_ref[:, s : s + 1]
        cb = wave_ref[:, :N]
        sb = wave_ref[:, N:]
        cosine = ca * cb - sa * sb
        sine = sa * cb + ca * sb
        for c in range(4):
            row = g * 16 + j * 4 + c
            real = v_ref[row : row + 1, :]
            imag = v_ref[row + 8 : row + 9, :]
            vg_ref[c, 0, s : s + 1, :] = real
            vg_ref[c, 1, s : s + 1, :] = imag
            mixed[c * 128 : (c + 1) * 128, s * N : (s + 1) * N] = (real * cosine - imag * sine).astype(BF16)
    d = lax.dot_general(q_ref[...], mixed[...], (((1,), (1,)), ((), ())), preferred_element_type=F32)
    for c in range(4):
        d_ref[pl.ds(c, 171, 4), :] = d[:, c * 128 : (c + 1) * 128]
    d_ref[684:704, :] = jnp.zeros((20, 128), F32)


def charge_part(v, charge, wave, ca, sa):
    return pl.pallas_call(
        charge_kernel,
        out_shape=(jax.ShapeDtypeStruct((4, 2, 16, N), F32), pltpu.VMEM((704, 128), F32)),
        in_specs=[pl.BlockSpec(memory_space=pltpu.VMEM)] * 5,
        out_specs=(pl.BlockSpec(memory_space=pltpu.VMEM),) * 2,
        scratch_shapes=[pltpu.VMEM((512, 4096), BF16)],
        name="charge_part",
    )(near(v), near(charge), near(wave), near(ca), near(sa))


def meet_kernel(in_ref, out_ref):
    out_ref[...] = (in_ref[0:176, :] + in_ref[176:352, :]) + (in_ref[352:528, :] + in_ref[528:704, :])


def met(arrived):
    return pl.pallas_call(
        meet_kernel,
        out_shape=pltpu.VMEM((176, 128), F32),
        in_specs=[pl.BlockSpec(memory_space=pltpu.VMEM)],
        out_specs=pl.BlockSpec(memory_space=pltpu.VMEM),
        name="meet",
    )(near(arrived))


def total_kernel(in_ref, out_ref, half):
    half[...] = in_ref[0:88, :] + in_ref[88:176, :]
    own = half[0:11, :]
    for m in range(1, 8):
        own = own + half[m * 11 : (m + 1) * 11, :]
    for m in range(16):
        out_ref[m * 11 : (m + 1) * 11, :] = own


def totals(arrived):
    return pl.pallas_call(
        total_kernel,
        out_shape=pltpu.VMEM((176, 128), F32),
        in_specs=[pl.BlockSpec(memory_space=pltpu.VMEM)],
        out_specs=pl.BlockSpec(memory_space=pltpu.VMEM),
        scratch_shapes=[pltpu.VMEM((88, 128), F32)],
        name="totals",
    )(near(arrived))


def copy_kernel(in_ref, out_ref):
    x = in_ref[...]
    for y in range(4):
        out_ref[y * 176 : (y + 1) * 176, :] = x


def four_copies(x):
    return pl.pallas_call(
        copy_kernel,
        out_shape=pltpu.VMEM((704, 128), F32),
        in_specs=[pl.BlockSpec(memory_space=pltpu.VMEM)],
        out_specs=pl.BlockSpec(memory_space=pltpu.VMEM),
        name="four_copies",
    )(near(x))


def near(x):
    return pltpu.with_memory_space_constraint(x, pltpu.VMEM)


def exchange(parts, axes):
    return lax.all_to_all(parts, axes, split_axis=0, concat_axis=0, tiled=True)


def tables():
    index = np.arange(N)
    flat = split_table(wave_table(index, index))
    y0, z4, zs, yp = np.meshgrid(np.arange(2), np.arange(4), np.arange(16), np.arange(2), indexing="ij")
    plane = (((2 * yp + y0) * 16 + zs) * 4 + z4).reshape(-1)
    line = split_table(wave_table(plane, index - N // 2) * float(N) ** -1.5)
    return flat, line


def body(potential, stick_mill, positions, aug_charge):
    (hi, lo), (line_hi, line_lo) = tables()
    hi, lo, line_hi, line_lo = map(jnp.asarray, (hi, lo, line_hi, line_lo))
    grp = lax.axis_index(GRP)
    fft = lax.axis_index(FFT)
    mine = lax.dynamic_slice_in_dim(stick_mill, fft * 16, 16, 1)
    part = plane_part(potential.reshape(512, N), stick_mill, grp.reshape(1), hi, lo)
    arrived = exchange(part.reshape(32, 8, 128), ROWS)
    lines = folded(arrived.reshape(256, 128))
    arrived = exchange(lines.reshape(16, 1, 256), "z")
    wave, ca, sa = phases(positions.T, mine, hi, lo)
    charge = aug_charge.reshape(171, 16 * N)
    arrived, charge, wave, ca, sa = lax.optimization_barrier((arrived, charge, wave, ca, sa))
    copies = line_part(arrived.reshape(32, 128), line_hi, line_lo)
    v = exchange(copies, GRP).reshape(128, N)
    vg, part = charge_part(v, charge, wave, ca, sa)
    arrived = exchange(part.reshape(4, 176, 128), "y")
    mid = met(arrived.reshape(704, 128))
    arrived = exchange(mid.reshape(16, 1, 1408), "z")
    own = totals(arrived.reshape(176, 128))
    line = exchange(own.reshape(16, 1, 1408), "z")
    whole = exchange(four_copies(line.reshape(176, 128)).reshape(4, 176, 128), "y")
    return vg, jnp.moveaxis(whole.reshape(176, 4, 128)[:171], 1, 0)


def solution(mesh):
    fine = Mesh(mesh.devices.reshape(4, 16, 4, 2), ("y", "z", "x", "core"))
    placed = (P(None, FFT, GRP, None), P(), P(None, GRP), P(None, FFT, None))
    return jax.shard_map(
        body,
        mesh=fine,
        in_specs=placed,
        out_specs=(P(None, None, FFT, None), P(None, None, GRP)),
        check_vma=False,
    )
```

```python
import math

import jax
import jax.numpy as jnp
import numpy as np
from jax import lax
from jax.experimental import pallas as pl
from jax.experimental.pallas import tpu as pltpu
from jax.sharding import Mesh
from jax.sharding import PartitionSpec as P

N = 256
H = 128
GRP = ("x", "core")
FFT = ("y", "zh", "zl")
F32 = jnp.float32
BF16 = jnp.bfloat16
VMEM = pl.BlockSpec(memory_space=pltpu.VMEM)


def split_table(table):
    high = table.astype(np.float32).astype(jnp.bfloat16)
    low = (table - high.astype(np.float64)).astype(np.float32).astype(jnp.bfloat16)
    return high, low


def wave_table(left, right):
    angle = 2.0 * math.pi / N * np.mod(np.outer(left, right), N)
    return np.concatenate([np.cos(angle), np.sin(angle)], axis=1)


def tables():
    index = np.arange(N)
    flat = split_table(wave_table(index, index[:H]))
    z4, f = np.meshgrid(np.arange(4), np.arange(64), indexing="ij")
    plane = (f * 4 + z4).reshape(-1)
    line = split_table(wave_table(plane, index - N // 2) * float(N) ** -1.5)
    return flat, line


def split_value(x):
    high = x.astype(BF16)
    return high, (x - high.astype(F32)).astype(BF16)


def dot(a, b):
    return jnp.dot(a, b, preferred_element_type=F32)


def near(x):
    return pltpu.with_memory_space_constraint(x, pltpu.VMEM)


def picks(index):
    grid = lax.broadcasted_iota(jnp.int32, (H, 1024), 0)
    hit = grid == jnp.abs(index)
    even = jnp.where(hit, 1.0, 0.0).astype(BF16)
    odd = jnp.where(hit, jnp.where(index < 0, -1.0, 1.0), 0.0).astype(BF16)
    return jnp.concatenate([even, even], axis=0), jnp.concatenate([odd, odd], axis=0)


def plane_kernel(grp_ref, pot_ref, mill_ref, hi_ref, lo_ref, out_ref, stack, turned):
    start = pl.multiple_of(grp_ref[0] * 32, 32)
    near_hi = hi_ref[pl.ds(start, 32), :]
    near_lo = lo_ref[pl.ds(start, 32), :]
    even_y, odd_y = picks(mill_ref[1:2, :])
    cos_y = dot(jnp.concatenate([near_hi[:, :H], near_lo[:, :H]], axis=1), even_y)
    sin_y = dot(jnp.concatenate([near_hi[:, H:], near_lo[:, H:]], axis=1), odd_y)
    even_x, odd_x = picks(mill_ref[0:1, :])
    hi = hi_ref[...]
    wide = jnp.concatenate([hi, lo_ref[...], hi], axis=0)
    for c in range(4):
        p_hi, p_lo = split_value(pot_ref[c * 128 : (c + 1) * 128, :])
        wave = dot(jnp.concatenate([p_hi, p_hi, p_lo], axis=1), wide)
        w_hi, w_lo = split_value(wave)
        even = dot(jnp.concatenate([w_hi[:, :H], w_lo[:, :H]], axis=1), even_x)
        odd = dot(jnp.concatenate([w_hi[:, H:], w_lo[:, H:]], axis=1), odd_x)
        for z in range(4):
            e = even[z * 32 : (z + 1) * 32, :]
            o = odd[z * 32 : (z + 1) * 32, :]
            real = jnp.sum(e * cos_y - o * sin_y, axis=0, keepdims=True)
            imag = -jnp.sum(e * sin_y + o * cos_y, axis=0, keepdims=True)
            for j in range(4):
                row = z * 32 + j * 4 + c
                stack[row : row + 1, :] = real
                stack[row + 16 : row + 17, :] = imag
    for b in range(8):
        turned[b * 128 : (b + 1) * 128, :] = stack[:, b * 128 : (b + 1) * 128].T
    lane = lax.broadcasted_iota(jnp.int32, (16, 128), 1)
    upper = jnp.bitwise_and(lane, 8) != 0
    second = jnp.bitwise_and(lane, 4) != 0
    for y in range(4):
        for x in range(4):
            base = y * 256 + x * 4
            parts = [turned[pl.ds(base + j, 16, 16), :] for j in range(4)]
            tile = jnp.where(upper, jnp.where(second, parts[3], parts[2]), jnp.where(second, parts[1], parts[0]))
            at = (y * 4 + x) * 16
            out_ref[at : at + 16, :] = tile


def plane_part(potential, stick_mill, grp, hi, lo):
    return pl.pallas_call(
        plane_kernel,
        out_shape=pltpu.VMEM((256, 128), F32),
        in_specs=[pl.BlockSpec(memory_space=pltpu.SMEM)] + [VMEM] * 4,
        out_specs=VMEM,
        scratch_shapes=[pltpu.VMEM((128, 1024), F32), pltpu.VMEM((1024, 128), F32)],
        name="plane_part",
    )(grp, potential, stick_mill, hi, lo)


def fold_kernel(in_ref, out_ref):
    for y in range(4):
        at = y * 64
        total = (in_ref[at : at + 16, :] + in_ref[at + 16 : at + 32, :]) + (
            in_ref[at + 32 : at + 48, :] + in_ref[at + 48 : at + 64, :]
        )
        for core in range(2):
            out_ref[pl.ds(core * 4 + y, 16, 8), :] = total


def folded(arrived):
    return pl.pallas_call(
        fold_kernel,
        out_shape=pltpu.VMEM((128, 128), F32),
        in_specs=[VMEM],
        out_specs=VMEM,
        name="fold",
    )(near(arrived))


def line_kernel(in_ref, hi_ref, lo_ref, out_ref):
    rows = [in_ref[pl.ds(y, 16, 8), :] + in_ref[pl.ds(y + 4, 16, 8), :] for y in range(4)]
    t = jnp.concatenate(rows + rows, axis=0).T
    lower = lax.broadcasted_iota(jnp.int32, (32, 128), 1) < 64
    halves = [jnp.where(lower, t[b * 64 : b * 64 + 32, :], t[b * 64 + 32 : b * 64 + 64, :]) for b in range(2)]
    a_hi, a_lo = split_value(jnp.concatenate(halves, axis=1))
    hi = hi_ref[...]
    r = dot(a_hi, hi) + dot(a_hi, lo_ref[...]) + dot(a_lo, hi)
    real = r[0:16, :N] + r[16:32, N:]
    imag = r[16:32, :N] - r[0:16, N:]
    for x in range(4):
        out_ref[x, 0:16, :] = real
        out_ref[x, 16:32, :] = imag


def line_part(arrived, hi, lo):
    return pl.pallas_call(
        line_kernel,
        out_shape=pltpu.VMEM((4, 32, N), F32),
        in_specs=[VMEM] * 3,
        out_specs=VMEM,
        name="line_part",
    )(near(arrived), near(hi), near(lo))


def phase_kernel(pos_ref, mill_ref, hi_ref, lo_ref, wave_ref, cos_ref, sin_ref):
    zcol = pos_ref[:, 2:3]
    grid = lax.broadcasted_iota(jnp.int32, (128, N), 1)
    pick = jnp.where(grid == zcol, 1.0, 0.0).astype(BF16)
    sign = 1.0 - 2.0 * jnp.bitwise_and(zcol, 1).astype(F32)
    wave = dot(pick, hi_ref[...]) + dot(pick, lo_ref[...])
    turn = wave * sign
    wave_ref[:, 0:H] = turn[:, :H]
    wave_ref[:, H:N] = wave[:, :H]
    wave_ref[:, N : N + H] = turn[:, H:]
    wave_ref[:, N + H :] = wave[:, H:]
    k = pos_ref[:, 0:1] * mill_ref[0:1, :] + pos_ref[:, 1:2] * mill_ref[1:2, :]
    angle = (2.0 * math.pi / N) * jnp.bitwise_and(k, N - 1).astype(F32)
    cos_ref[...] = jnp.cos(angle)
    sin_ref[...] = jnp.sin(angle)


def phases(pos_cols, mine, hi, lo):
    return pl.pallas_call(
        phase_kernel,
        out_shape=(
            pltpu.VMEM((128, 2 * N), F32),
            pltpu.VMEM((128, 16), F32),
            pltpu.VMEM((128, 16), F32),
        ),
        in_specs=[VMEM] * 4,
        out_specs=(VMEM,) * 3,
        name="phases",
    )(pos_cols, mine, hi, lo)


def charge_kernel(v_ref, far_ref, wave_ref, ca_ref, sa_ref, vg_ref, d_ref, mixed, q_ref, done):
    load = pltpu.make_async_copy(far_ref, q_ref, done)
    load.start()
    for s in range(16):
        ca = ca_ref[:, s : s + 1]
        sa = sa_ref[:, s : s + 1]
        cb = wave_ref[:, :N]
        sb = wave_ref[:, N:]
        cosine = ca * cb - sa * sb
        sine = sa * cb + ca * sb
        for c in range(4):
            row = (s // 4) * 32 + (s % 4) * 4 + c
            real = v_ref[row : row + 1, :]
            imag = v_ref[row + 16 : row + 17, :]
            vg_ref[c, 0, s : s + 1, :] = real
            vg_ref[c, 1, s : s + 1, :] = imag
            mixed[c * 128 : (c + 1) * 128, s * N : (s + 1) * N] = (real * cosine - imag * sine).astype(BF16)
    load.wait()
    d = lax.dot_general(q_ref[...], mixed[...], (((1,), (1,)), ((), ())), preferred_element_type=F32)
    for c in range(4):
        d_ref[pl.ds(c, 171, 4), :] = d[:, c * 128 : (c + 1) * 128]
    d_ref[684:704, :] = jnp.zeros((20, 128), F32)


def charge_part(v, charge, wave, ca, sa):
    return pl.pallas_call(
        charge_kernel,
        out_shape=(jax.ShapeDtypeStruct((4, 2, 16, N), F32), pltpu.VMEM((704, 128), F32)),
        in_specs=[VMEM, pl.BlockSpec(memory_space=pl.ANY), VMEM, VMEM, VMEM],
        out_specs=(VMEM,) * 2,
        scratch_shapes=[
            pltpu.VMEM((512, 4096), BF16),
            pltpu.VMEM((171, 4096), BF16),
            pltpu.SemaphoreType.DMA(()),
        ],
        name="charge_part",
    )(near(v), charge, near(wave), near(ca), near(sa))


def meet_kernel(in_ref, out_ref, half):
    total = in_ref[0:88, :]
    for m in range(1, 8):
        total = total + in_ref[m * 88 : (m + 1) * 88, :]
    half[...] = total
    own = half[0:44, :] + half[44:88, :]
    for m in range(4):
        out_ref[m * 44 : (m + 1) * 44, :] = own


def met(arrived):
    return pl.pallas_call(
        meet_kernel,
        out_shape=pltpu.VMEM((176, 128), F32),
        in_specs=[VMEM],
        out_specs=VMEM,
        scratch_shapes=[pltpu.VMEM((88, 128), F32)],
        name="meet",
    )(near(arrived))


def total_kernel(in_ref, out_ref, half):
    half[...] = in_ref[0:88, :] + in_ref[88:176, :]
    own = half[0:44, :] + half[44:88, :]
    half[0:44, :] = own
    half[44:88, :] = own
    pair = half[...]
    for m in range(8):
        out_ref[m * 88 : (m + 1) * 88, :] = pair


def totals(arrived):
    return pl.pallas_call(
        total_kernel,
        out_shape=pltpu.VMEM((704, 128), F32),
        in_specs=[VMEM],
        out_specs=VMEM,
        scratch_shapes=[pltpu.VMEM((88, 128), F32)],
        name="totals",
    )(near(arrived))


def exchange(parts, axes):
    return lax.all_to_all(parts, axes, split_axis=0, concat_axis=0, tiled=True)


def body(potential, stick_mill, positions, aug_charge):
    (hi, lo), (line_hi, line_lo) = tables()
    hi, lo, line_hi, line_lo = map(jnp.asarray, (hi, lo, line_hi, line_lo))
    grp = lax.axis_index(GRP)
    fft = lax.axis_index(FFT)
    mine = lax.dynamic_slice_in_dim(stick_mill, fft * 16, 16, 1)
    part = plane_part(potential.reshape(512, N), stick_mill, grp.reshape(1), hi, lo)
    arrived = exchange(part.reshape(16, 16, 128), ("y", "x"))
    lines = folded(arrived.reshape(256, 128))
    arrived = exchange(lines.reshape(32, 1, 512), ("zh", "zl", "core"))
    wave, ca, sa = phases(positions.T, mine, hi, lo)
    charge = aug_charge.reshape(171, 16 * N)
    arrived, charge, wave, ca, sa = lax.optimization_barrier((arrived, charge, wave, ca, sa))
    copies = line_part(arrived.reshape(128, 128), line_hi, line_lo)
    v = exchange(copies, "x").reshape(128, N)
    vg, part = charge_part(v, charge, wave, ca, sa)
    arrived = exchange(part.reshape(16, 1, 5632), ("y", "zl"))
    mid = met(arrived.reshape(704, 128))
    arrived = exchange(mid.reshape(4, 1, 5632), "zh")
    own = totals(arrived.reshape(176, 128))
    whole = exchange(own.reshape(16, 1, 5632), ("y", "zl"))
    return vg, jnp.moveaxis(whole.reshape(176, 4, 128)[:171], 1, 0)


def solution(mesh):
    fine = Mesh(mesh.devices.reshape(4, 4, 4, 4, 2), ("y", "zh", "zl", "x", "core"))
    placed = (P(None, FFT, GRP, None), P(), P(None, GRP), P(None, FFT, None))
    return jax.shard_map(
        body,
        mesh=fine,
        in_specs=placed,
        out_specs=(P(None, None, FFT, None), P(None, None, GRP)),
        check_vma=False,
    )
```

```python
import math

import jax
import jax.numpy as jnp
import numpy as np
from jax import lax
from jax.experimental import pallas as pl
from jax.experimental.pallas import tpu as pltpu
from jax.sharding import Mesh
from jax.sharding import PartitionSpec as P

N = 256
H = 128
GRP = ("x", "core")
FFT = ("y", "zh", "zl")
F32 = jnp.float32
BF16 = jnp.bfloat16
VMEM = pl.BlockSpec(memory_space=pltpu.VMEM)


def split_table(table):
    high = table.astype(np.float32).astype(jnp.bfloat16)
    low = (table - high.astype(np.float64)).astype(np.float32).astype(jnp.bfloat16)
    return high, low


def wave_table(left, right):
    angle = 2.0 * math.pi / N * np.mod(np.outer(left, right), N)
    return np.concatenate([np.cos(angle), np.sin(angle)], axis=1)


def tables():
    index = np.arange(N)
    flat = split_table(wave_table(index, index[:H]))
    z4, f = np.meshgrid(np.arange(4), np.arange(64), indexing="ij")
    plane = (f * 4 + z4).reshape(-1)
    line = split_table(wave_table(plane, index - N // 2) * float(N) ** -1.5)
    return flat, line


def split_value(x):
    high = x.astype(BF16)
    return high, (x - high.astype(F32)).astype(BF16)


def dot(a, b):
    return jnp.dot(a, b, preferred_element_type=F32)


def near(x):
    return pltpu.with_memory_space_constraint(x, pltpu.VMEM)


def picks(index):
    grid = lax.broadcasted_iota(jnp.int32, (H, 1024), 0)
    hit = grid == jnp.abs(index)
    even = jnp.where(hit, 1.0, 0.0).astype(BF16)
    odd = jnp.where(hit, jnp.where(index < 0, -1.0, 1.0), 0.0).astype(BF16)
    return jnp.concatenate([even, even], axis=0), jnp.concatenate([odd, odd], axis=0)


def place(axes):
    return lax.axis_index(axes)


def plane_kernel(pot_ref, mill_ref, pos_ref, hi_ref, lo_ref, out_ref, wave_ref, cos_ref, sin_ref, *scratch):
    pot, mill, pos, hi, lo, chosen, turned, sems = scratch
    loads = [
        pltpu.make_async_copy(mill_ref, mill, sems.at[0]),
        pltpu.make_async_copy(pos_ref, pos, sems.at[1]),
        pltpu.make_async_copy(hi_ref, hi, sems.at[2]),
        pltpu.make_async_copy(lo_ref, lo, sems.at[3]),
    ]
    chunks = [
        pltpu.make_async_copy(pot_ref.at[:, pl.ds(8 * q, 8), pl.ds(h * H, H)], pot.at[q, h], sems.at[4 + 2 * q + h])
        for q in range(4)
        for h in range(2)
    ]
    for load in loads + chunks:
        load.start()
    grp = place(GRP)
    fft = place(FFT)
    loads[0].wait()
    even_x, odd_x = picks(mill[0:1, :])
    even_y, odd_y = picks(mill[1:2, :])
    loads[1].wait()
    cols = jnp.concatenate([pos[...].astype(F32), jnp.zeros((125, 128), F32)], axis=0).T
    block = pl.multiple_of((fft >> 3) * 128, 128)
    shift = (128 - (fft & 7) * 16) & 127
    near_mill = jnp.concatenate([mill[:, pl.ds(block, 128)].astype(F32), jnp.zeros((6, 128), F32)], axis=0)
    mine = pltpu.roll(near_mill, shift, 1)
    k = (cols[:, 0:1] * mine[0:1, :] + cols[:, 1:2] * mine[1:2, :]).astype(jnp.int32)
    angle = (2.0 * math.pi / N) * jnp.bitwise_and(k, N - 1).astype(F32)
    cos_ref[...] = jnp.cos(angle)
    sin_ref[...] = jnp.sin(angle)
    zcol = cols[:, 2:3].astype(jnp.int32)
    grid = lax.broadcasted_iota(jnp.int32, (128, N), 1)
    pick = jnp.where(grid == zcol, 1.0, 0.0).astype(BF16)
    sign = 1.0 - 2.0 * jnp.bitwise_and(zcol, 1).astype(F32)
    loads[2].wait()
    loads[3].wait()
    wave = dot(pick, hi[...]) + dot(pick, lo[...])
    turn = wave * sign
    wave_ref[:, 0:H] = turn[:, :H]
    wave_ref[:, H:N] = wave[:, :H]
    wave_ref[:, N : N + H] = turn[:, H:]
    wave_ref[:, N + H :] = wave[:, H:]

    start = pl.multiple_of(grp * 32, 32)
    near_hi = hi[pl.ds(start, 32), :]
    near_lo = lo[pl.ds(start, 32), :]
    cos_y = dot(jnp.concatenate([near_hi[:, :H], near_lo[:, :H]], axis=1), even_y)
    sin_y = dot(jnp.concatenate([near_hi[:, H:], near_lo[:, H:]], axis=1), odd_y)
    wide = jnp.concatenate([hi[...], lo[...], hi[...]], axis=0)
    for q in range(4):
        halves = []
        for h in range(2):
            chunks[2 * q + h].wait()
            rows = pot.at[q, h].reshape(128, H)
            halves.append(jnp.concatenate([rows[pl.ds(y, 16, 8), :] for y in range(8)], axis=0))
        x = jnp.concatenate(halves, axis=1)
        p_hi, p_lo = split_value(x)
        w_hi, w_lo = split_value(dot(jnp.concatenate([p_hi, p_hi, p_lo], axis=1), wide))
        at = q * 128
        chosen[0, at : at + 128, 0:H] = w_hi[:, :H]
        chosen[0, at : at + 128, H:N] = w_lo[:, :H]
        chosen[1, at : at + 128, 0:H] = w_hi[:, H:]
        chosen[1, at : at + 128, H:N] = w_lo[:, H:]
    for b in range(4):
        at = b * N
        even = dot(chosen[0], even_x[:, at : at + N])
        odd = dot(chosen[1], odd_x[:, at : at + N])
        real = jnp.zeros((16, N), F32)
        imag = jnp.zeros((16, N), F32)
        for y in range(32):
            e = even[y * 16 : (y + 1) * 16, :]
            o = odd[y * 16 : (y + 1) * 16, :]
            cy = cos_y[y : y + 1, at : at + N]
            sy = sin_y[y : y + 1, at : at + N]
            real = real + (e * cy - o * sy)
            imag = imag - (e * sy + o * cy)
        for h in range(2):
            part = jnp.concatenate([real[:, h * H : (h + 1) * H], imag[:, h * H : (h + 1) * H]], axis=0)
            turned[at + h * H : at + (h + 1) * H, :] = jnp.concatenate([part] * 4, axis=0).T
    lane = lax.broadcasted_iota(jnp.int32, (16, 128), 1)
    for y in range(4):
        for x in range(4):
            base = y * 256 + x * 4
            parts = [turned[pl.ds(base + j, 16, 16), :] for j in range(4)]
            low = jnp.where(lane < 32, parts[0], parts[1])
            high = jnp.where(lane < 96, parts[2], parts[3])
            at = (y * 4 + x) * 16
            out_ref[at : at + 16, :] = jnp.where(lane < 64, low, high)


def plane_part(potential, stick_mill, positions, hi, lo):
    return pl.pallas_call(
        plane_kernel,
        out_shape=(
            pltpu.VMEM((256, 128), F32),
            pltpu.VMEM((128, 2 * N), F32),
            pltpu.VMEM((128, 128), F32),
            pltpu.VMEM((128, 128), F32),
        ),
        in_specs=[pl.BlockSpec(memory_space=pl.ANY)] * 5,
        out_specs=(VMEM,) * 4,
        scratch_shapes=[
            pltpu.VMEM((4, 2, 16, 8, H), F32),
            pltpu.VMEM((2, 1024), jnp.int32),
            pltpu.VMEM((3, 128), jnp.int32),
            pltpu.VMEM((N, N), BF16),
            pltpu.VMEM((N, N), BF16),
            pltpu.VMEM((2, 512, N), BF16),
            pltpu.VMEM((1024, 128), F32),
            pltpu.SemaphoreType.DMA((12,)),
        ],
        name="plane_part",
    )(potential, stick_mill, positions, hi, lo)


def fold_kernel(in_ref, out_ref):
    for y in range(4):
        at = y * 64
        total = (in_ref[at : at + 16, :] + in_ref[at + 16 : at + 32, :]) + (
            in_ref[at + 32 : at + 48, :] + in_ref[at + 48 : at + 64, :]
        )
        for core in range(2):
            out_ref[pl.ds(core * 4 + y, 16, 8), :] = total


def folded(arrived):
    return pl.pallas_call(
        fold_kernel,
        out_shape=pltpu.VMEM((128, 128), F32),
        in_specs=[VMEM],
        out_specs=VMEM,
        name="fold",
    )(near(arrived))


def line_kernel(in_ref, hi_ref, lo_ref, out_ref, turned):
    rows = [in_ref[pl.ds(y, 16, 8), :] + in_ref[pl.ds(y + 4, 16, 8), :] for y in range(4)]
    turned[...] = jnp.concatenate(rows + rows, axis=0).T
    lower = lax.broadcasted_iota(jnp.int32, (32, 128), 1) < 64
    halves = [jnp.where(lower, turned[pl.ds(2 * b, 32, 4), :], turned[pl.ds(2 * b + 1, 32, 4), :]) for b in range(2)]
    a_hi, a_lo = split_value(jnp.concatenate(halves, axis=1))
    hi = hi_ref[...]
    r = dot(a_hi, hi) + dot(a_hi, lo_ref[...]) + dot(a_lo, hi)
    first = lax.broadcasted_iota(jnp.int32, (8, N), 0) < 4
    for j in range(4):
        own = r[j * 8 : j * 8 + 8, :N]
        other = pltpu.roll(r[j * 8 : j * 8 + 8, N:], 4, 0)
        v = own + jnp.where(first, other, -other)
        for x in range(4):
            out_ref[x, j * 8 : j * 8 + 8, :] = v


def line_part(arrived, hi, lo):
    return pl.pallas_call(
        line_kernel,
        out_shape=pltpu.VMEM((4, 32, N), F32),
        in_specs=[VMEM] * 3,
        out_specs=VMEM,
        scratch_shapes=[pltpu.VMEM((128, 128), F32)],
        name="line_part",
    )(near(arrived), near(hi), near(lo))


def charge_kernel(v_ref, q_ref, wave_ref, ca_ref, sa_ref, vg_ref, d_ref, mixed):
    for s in range(16):
        top = s * 8
        for c in range(4):
            vg_ref[c, 0, s : s + 1, :] = v_ref[top + c : top + c + 1, :]
            vg_ref[c, 1, s : s + 1, :] = v_ref[top + 4 + c : top + 5 + c, :]
        for a in range(0, 128, 16):
            ca = ca_ref[a : a + 16, s : s + 1]
            sa = sa_ref[a : a + 16, s : s + 1]
            cb = wave_ref[a : a + 16, :N]
            sb = wave_ref[a : a + 16, N:]
            cosine = ca * cb - sa * sb
            sine = sa * cb + ca * sb
            for c in range(4):
                real = v_ref[top + c : top + c + 1, :]
                imag = v_ref[top + 4 + c : top + 5 + c, :]
                mixed[c * 128 + a : c * 128 + a + 16, s * N : (s + 1) * N] = (real * cosine - imag * sine).astype(BF16)
    d = lax.dot_general(q_ref[...], mixed[...], (((1,), (1,)), ((), ())), preferred_element_type=F32)
    for c in range(4):
        d_ref[pl.ds(c, 171, 4), :] = d[:, c * 128 : (c + 1) * 128]
    d_ref[684:704, :] = jnp.zeros((20, 128), F32)


def charge_part(v, charge, wave, ca, sa):
    return pl.pallas_call(
        charge_kernel,
        out_shape=(jax.ShapeDtypeStruct((4, 2, 16, N), F32), pltpu.VMEM((704, 128), F32)),
        in_specs=[VMEM] * 5,
        out_specs=(VMEM,) * 2,
        scratch_shapes=[pltpu.VMEM((512, 4096), BF16)],
        name="charge_part",
    )(near(v), near(charge), near(wave), near(ca), near(sa))


def meet_kernel(in_ref, out_ref, half):
    total = in_ref[0:88, :]
    for m in range(1, 8):
        total = total + in_ref[m * 88 : (m + 1) * 88, :]
    half[...] = total
    own = half[0:44, :] + half[44:88, :]
    for m in range(4):
        out_ref[m * 44 : (m + 1) * 44, :] = own


def met(arrived):
    return pl.pallas_call(
        meet_kernel,
        out_shape=pltpu.VMEM((176, 128), F32),
        in_specs=[VMEM],
        out_specs=VMEM,
        scratch_shapes=[pltpu.VMEM((88, 128), F32)],
        name="meet",
    )(near(arrived))


def total_kernel(in_ref, out_ref, half):
    half[...] = in_ref[0:88, :] + in_ref[88:176, :]
    own = half[0:44, :] + half[44:88, :]
    half[0:44, :] = own
    half[44:88, :] = own
    pair = half[...]
    for m in range(8):
        out_ref[m * 88 : (m + 1) * 88, :] = pair


def totals(arrived):
    return pl.pallas_call(
        total_kernel,
        out_shape=pltpu.VMEM((704, 128), F32),
        in_specs=[VMEM],
        out_specs=VMEM,
        scratch_shapes=[pltpu.VMEM((88, 128), F32)],
        name="totals",
    )(near(arrived))


def exchange(parts, axes):
    return lax.all_to_all(parts, axes, split_axis=0, concat_axis=0, tiled=True)


def body(potential, stick_mill, positions, aug_charge):
    (hi, lo), (line_hi, line_lo) = tables()
    hi, lo, line_hi, line_lo = map(jnp.asarray, (hi, lo, line_hi, line_lo))
    part, wave, ca, sa = plane_part(potential.reshape(16, 32, N), stick_mill, positions, hi, lo)
    arrived = exchange(part.reshape(16, 16, 128), ("y", "x"))
    lines = folded(arrived.reshape(256, 128))
    arrived = exchange(lines.reshape(32, 1, 512), ("zh", "zl", "core"))
    copies = line_part(arrived.reshape(128, 128), line_hi, line_lo)
    v = exchange(copies, "x").reshape(128, N)
    v, aug_charge = lax.optimization_barrier((v, aug_charge))
    charge = aug_charge.reshape(171, 16 * N)
    vg, part = charge_part(v, charge, wave, ca, sa)
    arrived = exchange(part.reshape(16, 1, 5632), ("y", "zl"))
    mid = met(arrived.reshape(704, 128))
    arrived = exchange(mid.reshape(4, 1, 5632), "zh")
    own = totals(arrived.reshape(176, 128))
    whole = exchange(own.reshape(16, 1, 5632), ("y", "zl"))
    return vg, jnp.moveaxis(whole.reshape(176, 4, 128)[:171], 1, 0)


def solution(mesh):
    fine = Mesh(mesh.devices.reshape(4, 4, 4, 4, 2), ("y", "zh", "zl", "x", "core"))
    placed = (P(None, FFT, GRP, None), P(), P(None, GRP), P(None, FFT, None))
    return jax.shard_map(
        body,
        mesh=fine,
        in_specs=placed,
        out_specs=(P(None, None, FFT, None), P(None, None, GRP)),
        check_vma=False,
    )
```

```python
import math

import jax
import jax.numpy as jnp
import numpy as np
from jax import lax
from jax.experimental import pallas as pl
from jax.experimental.pallas import tpu as pltpu
from jax.sharding import Mesh
from jax.sharding import PartitionSpec as P

N = 256
H = 128
GRP = ("x", "core")
FFT = ("y", "zh", "zl")
F32 = jnp.float32
BF16 = jnp.bfloat16
VMEM = pl.BlockSpec(memory_space=pltpu.VMEM)


def split_table(table):
    high = table.astype(np.float32).astype(jnp.bfloat16)
    low = (table - high.astype(np.float64)).astype(np.float32).astype(jnp.bfloat16)
    return high, low


def wave_table(left, right):
    angle = 2.0 * math.pi / N * np.mod(np.outer(left, right), N)
    return np.concatenate([np.cos(angle), np.sin(angle)], axis=1)


def tables():
    index = np.arange(N)
    flat = split_table(wave_table(index, index[:H]))
    z4, f = np.meshgrid(np.arange(4), np.arange(64), indexing="ij")
    f = f // 16 * 16 + (f + 8) % 16
    plane = (f * 4 + z4).reshape(-1)
    line = split_table(wave_table(plane, index - N // 2) * float(N) ** -1.5)
    return flat, line


def split_value(x):
    high = x.astype(BF16)
    return high, (x - high.astype(F32)).astype(BF16)


def dot(a, b):
    return jnp.dot(a, b, preferred_element_type=F32)


def near(x):
    return pltpu.with_memory_space_constraint(x, pltpu.VMEM)


def picks(index):
    grid = lax.broadcasted_iota(jnp.int32, (H, 1024), 0)
    hit = grid == jnp.abs(index)
    even = jnp.where(hit, 1.0, 0.0).astype(BF16)
    odd = jnp.where(hit, jnp.where(index < 0, -1.0, 1.0), 0.0).astype(BF16)
    return jnp.concatenate([even, even], axis=0), jnp.concatenate([odd, odd], axis=0)


def place(axes):
    return lax.axis_index(axes)


def plane_kernel(pot_ref, mill_ref, pos_ref, hi_ref, lo_ref, out_ref, wave_ref, cos_ref, sin_ref, *scratch):
    pot, mill, pos, hi, lo, chosen, turned, sems = scratch
    loads = [
        pltpu.make_async_copy(mill_ref, mill, sems.at[0]),
        pltpu.make_async_copy(pos_ref, pos, sems.at[1]),
        pltpu.make_async_copy(hi_ref, hi, sems.at[2]),
        pltpu.make_async_copy(lo_ref, lo, sems.at[3]),
    ]
    chunks = [
        pltpu.make_async_copy(pot_ref.at[:, pl.ds(8 * q, 8), pl.ds(h * H, H)], pot.at[q, h], sems.at[4 + 2 * q + h])
        for q in range(4)
        for h in range(2)
    ]
    for load in loads + chunks:
        load.start()
    grp = place(GRP)
    fft = place(FFT)
    loads[0].wait()
    even_x, odd_x = picks(mill[0:1, :])
    even_y, odd_y = picks(mill[1:2, :])
    loads[1].wait()
    cols = jnp.concatenate([pos[...].astype(F32), jnp.zeros((125, 128), F32)], axis=0).T
    block = pl.multiple_of((fft >> 3) * 128, 128)
    shift = (128 - (fft & 7) * 16) & 127
    near_mill = jnp.concatenate([mill[:, pl.ds(block, 128)].astype(F32), jnp.zeros((6, 128), F32)], axis=0)
    mine = pltpu.roll(near_mill, shift, 1)
    k = (cols[:, 0:1] * mine[0:1, :] + cols[:, 1:2] * mine[1:2, :]).astype(jnp.int32)
    angle = (2.0 * math.pi / N) * jnp.bitwise_and(k, N - 1).astype(F32)
    cos_ref[...] = jnp.cos(angle)
    sin_ref[...] = jnp.sin(angle)
    zcol = cols[:, 2:3].astype(jnp.int32)
    grid = lax.broadcasted_iota(jnp.int32, (128, N), 1)
    pick = jnp.where(grid == zcol, 1.0, 0.0).astype(BF16)
    sign = 1.0 - 2.0 * jnp.bitwise_and(zcol, 1).astype(F32)
    loads[2].wait()
    loads[3].wait()
    wave = dot(pick, hi[...]) + dot(pick, lo[...])
    turn = wave * sign
    wave_ref[:, 0:H] = turn[:, :H]
    wave_ref[:, H:N] = wave[:, :H]
    wave_ref[:, N : N + H] = turn[:, H:]
    wave_ref[:, N + H :] = wave[:, H:]

    start = pl.multiple_of(grp * 32, 32)
    near_hi = hi[pl.ds(start, 32), :]
    near_lo = lo[pl.ds(start, 32), :]
    cos_y = dot(jnp.concatenate([near_hi[:, :H], near_lo[:, :H]], axis=1), even_y)
    sin_y = dot(jnp.concatenate([near_hi[:, H:], near_lo[:, H:]], axis=1), odd_y)
    wide = jnp.concatenate([hi[...], lo[...], hi[...]], axis=0)
    for q in range(4):
        halves = []
        for h in range(2):
            chunks[2 * q + h].wait()
            rows = pot.at[q, h].reshape(128, H)
            halves.append(jnp.concatenate([rows[pl.ds(y, 16, 8), :] for y in range(8)], axis=0))
        x = jnp.concatenate(halves, axis=1)
        p_hi, p_lo = split_value(x)
        w_hi, w_lo = split_value(dot(jnp.concatenate([p_hi, p_hi, p_lo], axis=1), wide))
        at = q * 128
        chosen[0, at : at + 128, 0:H] = w_hi[:, :H]
        chosen[0, at : at + 128, H:N] = w_lo[:, :H]
        chosen[1, at : at + 128, 0:H] = w_hi[:, H:]
        chosen[1, at : at + 128, H:N] = w_lo[:, H:]
    for b in range(4):
        at = b * N
        even = dot(chosen[0], even_x[:, at : at + N])
        odd = dot(chosen[1], odd_x[:, at : at + N])
        real = jnp.zeros((16, N), F32)
        imag = jnp.zeros((16, N), F32)
        for y in range(32):
            e = even[y * 16 : (y + 1) * 16, :]
            o = odd[y * 16 : (y + 1) * 16, :]
            cy = cos_y[y : y + 1, at : at + N]
            sy = sin_y[y : y + 1, at : at + N]
            real = real + (e * cy - o * sy)
            imag = imag - (e * sy + o * cy)
        for h in range(2):
            part = jnp.concatenate([real[:, h * H : (h + 1) * H], imag[:, h * H : (h + 1) * H]], axis=0)
            turned[at + h * H : at + (h + 1) * H, :] = jnp.concatenate([part] * 4, axis=0).T
    lane = lax.broadcasted_iota(jnp.int32, (16, 128), 1)
    for y in range(4):
        for x in range(4):
            base = y * 256 + x * 4
            parts = [turned[pl.ds(base + j, 16, 16), :] for j in range(4)]
            low = jnp.where(lane < 32, parts[0], parts[1])
            high = jnp.where(lane < 96, parts[2], parts[3])
            at = (y * 4 + x) * 16
            out_ref[at : at + 16, :] = jnp.where(lane < 64, low, high)


def plane_part(potential, stick_mill, positions, hi, lo):
    return pl.pallas_call(
        plane_kernel,
        out_shape=(
            pltpu.VMEM((256, 128), F32),
            pltpu.VMEM((128, 2 * N), F32),
            pltpu.VMEM((128, 128), F32),
            pltpu.VMEM((128, 128), F32),
        ),
        in_specs=[pl.BlockSpec(memory_space=pl.ANY)] * 5,
        out_specs=(VMEM,) * 4,
        scratch_shapes=[
            pltpu.VMEM((4, 2, 16, 8, H), F32),
            pltpu.VMEM((2, 1024), jnp.int32),
            pltpu.VMEM((3, 128), jnp.int32),
            pltpu.VMEM((N, N), BF16),
            pltpu.VMEM((N, N), BF16),
            pltpu.VMEM((2, 512, N), BF16),
            pltpu.VMEM((1024, 128), F32),
            pltpu.SemaphoreType.DMA((12,)),
        ],
        name="plane_part",
    )(potential, stick_mill, positions, hi, lo)


def fold_kernel(in_ref, out_ref):
    for y in range(4):
        at = y * 64
        total = (in_ref[at : at + 16, :] + in_ref[at + 16 : at + 32, :]) + (
            in_ref[at + 32 : at + 48, :] + in_ref[at + 48 : at + 64, :]
        )
        for core in range(2):
            out_ref[pl.ds(core * 4 + y, 8, 8), :] = total[8:16, :]
            out_ref[pl.ds(64 + core * 4 + y, 8, 8), :] = total[0:8, :]


def folded(arrived):
    return pl.pallas_call(
        fold_kernel,
        out_shape=pltpu.VMEM((128, 128), F32),
        in_specs=[VMEM],
        out_specs=VMEM,
        name="fold",
    )(near(arrived))


def line_kernel(in_ref, hi_ref, lo_ref, out_ref, turned):
    rows = [in_ref[pl.ds(y, 16, 8), :] + in_ref[pl.ds(y + 4, 16, 8), :] for y in range(4)]
    turned[...] = jnp.concatenate(rows + rows, axis=0).T
    lower = lax.broadcasted_iota(jnp.int32, (32, 128), 1) < 64
    halves = [jnp.where(lower, turned[pl.ds(2 * b, 32, 4), :], turned[pl.ds(2 * b + 1, 32, 4), :]) for b in range(2)]
    a_hi, a_lo = split_value(jnp.concatenate(halves, axis=1))
    hi = hi_ref[...]
    r = dot(a_hi, hi) + dot(a_hi, lo_ref[...]) + dot(a_lo, hi)
    first = lax.broadcasted_iota(jnp.int32, (8, N), 0) < 4
    for j in range(4):
        own = r[j * 8 : j * 8 + 8, :N]
        other = pltpu.roll(r[j * 8 : j * 8 + 8, N:], 4, 0)
        v = own + jnp.where(first, other, -other)
        for x in range(4):
            out_ref[x, j * 8 : j * 8 + 8, :] = v


def line_part(arrived, hi, lo):
    return pl.pallas_call(
        line_kernel,
        out_shape=pltpu.VMEM((4, 32, N), F32),
        in_specs=[VMEM] * 3,
        out_specs=VMEM,
        scratch_shapes=[pltpu.VMEM((128, 128), F32)],
        name="line_part",
    )(near(arrived), near(hi), near(lo))


def charge_kernel(v_ref, q_ref, wave_ref, ca_ref, sa_ref, vg_ref, d_ref, mixed):
    for s in range(16):
        top = s * 8
        for c in range(4):
            vg_ref[c, 0, s : s + 1, :] = v_ref[top + c : top + c + 1, :]
            vg_ref[c, 1, s : s + 1, :] = v_ref[top + 4 + c : top + 5 + c, :]
        for a in range(0, 128, 16):
            ca = ca_ref[a : a + 16, s : s + 1]
            sa = sa_ref[a : a + 16, s : s + 1]
            cb = wave_ref[a : a + 16, :N]
            sb = wave_ref[a : a + 16, N:]
            cosine = ca * cb - sa * sb
            sine = sa * cb + ca * sb
            for c in range(4):
                real = v_ref[top + c : top + c + 1, :]
                imag = v_ref[top + 4 + c : top + 5 + c, :]
                mixed[c * 128 + a : c * 128 + a + 16, s * N : (s + 1) * N] = (real * cosine - imag * sine).astype(BF16)
    d = lax.dot_general(q_ref[...], mixed[...], (((1,), (1,)), ((), ())), preferred_element_type=F32)
    for c in range(4):
        d_ref[pl.ds(c, 171, 4), :] = d[:, c * 128 : (c + 1) * 128]
    d_ref[684:704, :] = jnp.zeros((20, 128), F32)


def charge_part(v, charge, wave, ca, sa):
    return pl.pallas_call(
        charge_kernel,
        out_shape=(jax.ShapeDtypeStruct((4, 2, 16, N), F32), pltpu.VMEM((704, 128), F32)),
        in_specs=[VMEM] * 5,
        out_specs=(VMEM,) * 2,
        scratch_shapes=[pltpu.VMEM((512, 4096), BF16)],
        name="charge_part",
    )(near(v), near(charge), near(wave), near(ca), near(sa))


def meet_kernel(in_ref, out_ref, half):
    total = in_ref[0:88, :]
    for m in range(1, 8):
        total = total + in_ref[m * 88 : (m + 1) * 88, :]
    half[...] = total
    own = half[0:44, :] + half[44:88, :]
    for m in range(4):
        out_ref[m * 44 : (m + 1) * 44, :] = own


def met(arrived):
    return pl.pallas_call(
        meet_kernel,
        out_shape=pltpu.VMEM((176, 128), F32),
        in_specs=[VMEM],
        out_specs=VMEM,
        scratch_shapes=[pltpu.VMEM((88, 128), F32)],
        name="meet",
    )(near(arrived))


def total_kernel(in_ref, out_ref, half):
    half[...] = in_ref[0:88, :] + in_ref[88:176, :]
    own = half[0:44, :] + half[44:88, :]
    half[0:44, :] = own
    half[44:88, :] = own
    pair = half[...]
    for m in range(8):
        out_ref[m * 88 : (m + 1) * 88, :] = pair


def totals(arrived):
    return pl.pallas_call(
        total_kernel,
        out_shape=pltpu.VMEM((704, 128), F32),
        in_specs=[VMEM],
        out_specs=VMEM,
        scratch_shapes=[pltpu.VMEM((88, 128), F32)],
        name="totals",
    )(near(arrived))


def exchange(parts, axes, members=None):
    groups = None if members is None else [members]
    return lax.all_to_all(parts, axes, split_axis=0, concat_axis=0, tiled=True, axis_index_groups=groups)


def body(potential, stick_mill, positions, aug_charge):
    (hi, lo), (line_hi, line_lo) = tables()
    hi, lo, line_hi, line_lo = map(jnp.asarray, (hi, lo, line_hi, line_lo))
    part, wave, ca, sa = plane_part(potential.reshape(16, 32, N), stick_mill, positions, hi, lo)
    arrived = exchange(part.reshape(16, 16, 128), ("y", "x"))
    lines = folded(arrived.reshape(256, 128))
    arrived = exchange(lines.reshape(32, 1, 512), ("zh", "zl", "core"), [(i + 16) % 32 for i in range(32)])
    copies = line_part(arrived.reshape(128, 128), line_hi, line_lo)
    v = exchange(copies, "x").reshape(128, N)
    v, aug_charge = lax.optimization_barrier((v, aug_charge))
    charge = aug_charge.reshape(171, 16 * N)
    vg, part = charge_part(v, charge, wave, ca, sa)
    arrived = exchange(part.reshape(16, 1, 5632), ("y", "zl"))
    mid = met(arrived.reshape(704, 128))
    arrived = exchange(mid.reshape(4, 1, 5632), "zh", [2, 3, 0, 1])
    own = totals(arrived.reshape(176, 128))
    whole = exchange(own.reshape(16, 1, 5632), ("y", "zl"))
    return vg, jnp.moveaxis(whole.reshape(176, 4, 128)[:171], 1, 0)


def solution(mesh):
    fine = Mesh(mesh.devices.reshape(4, 4, 4, 4, 2), ("y", "zh", "zl", "x", "core"))
    placed = (P(None, FFT, GRP, None), P(), P(None, GRP), P(None, FFT, None))
    return jax.shard_map(
        body,
        mesh=fine,
        in_specs=placed,
        out_specs=(P(None, None, FFT, None), P(None, None, GRP)),
        check_vma=False,
    )
```

```python
import math

import jax
import jax.numpy as jnp
import numpy as np
from jax import lax
from jax.experimental import pallas as pl
from jax.experimental.pallas import tpu as pltpu
from jax.sharding import Mesh
from jax.sharding import PartitionSpec as P

N = 256
H = 128
GRP = ("x", "core")
FFT = ("y", "zh", "zl")
F32 = jnp.float32
BF16 = jnp.bfloat16
VMEM = pl.BlockSpec(memory_space=pltpu.VMEM)

FIRST = 10
LINE = [2 * ((FIRST + i) % 16) + core for i in range(16) for core in (1, 0)]
FAR = [[1, 6, 8, 12], [0, 5, 9, 14], [2, 4, 10, 15], [3, 7, 11, 13]]
LEADS = [8, 9, 10, 11]
NEAR = [[16 * y + four[b] for four in FAR for y in range(4)] for b in range(4)]
CROSS = [[16 * y + z for z in [lead] + [z for z in four if z != lead]] for four, lead in zip(FAR, LEADS) for y in range(4)]


def split_table(table):
    high = table.astype(np.float32).astype(jnp.bfloat16)
    low = (table - high.astype(np.float64)).astype(np.float32).astype(jnp.bfloat16)
    return high, low


def wave_table(left, right):
    angle = 2.0 * math.pi / N * np.mod(np.outer(left, right), N)
    return np.concatenate([np.cos(angle), np.sin(angle)], axis=1)


def tables():
    index = np.arange(N)
    flat = split_table(wave_table(index, index[:H]))
    z4, f = np.meshgrid(np.arange(4), np.arange(64), indexing="ij")
    f = f // 16 * 16 + (f + FIRST) % 16
    plane = (f * 4 + z4).reshape(-1)
    line = split_table(wave_table(plane, index - N // 2) * float(N) ** -1.5)
    return flat, line


def split_value(x):
    high = x.astype(BF16)
    return high, (x - high.astype(F32)).astype(BF16)


def dot(a, b):
    return jnp.dot(a, b, preferred_element_type=F32)


def fitted(values, degree=8):
    fit = np.polynomial.chebyshev.Chebyshev.interpolate(lambda w: values(np.sqrt(w)), degree, domain=[0.0, 1.0])
    return [float(c) for c in fit.convert(kind=np.polynomial.Polynomial).coef]


def turn_of(k):
    u = (k - H).astype(F32) * (1.0 / H)
    w = u * u
    even = fitted(lambda r: -np.cos(math.pi * r))
    odd = fitted(lambda r: -math.pi * np.sinc(r))
    cosine = jnp.full_like(u, even[-1])
    sine = jnp.full_like(u, odd[-1])
    for e, o in zip(even[-2::-1], odd[-2::-1]):
        cosine = cosine * w + e
        sine = sine * w + o
    return cosine, sine * u


def near(x):
    return pltpu.with_memory_space_constraint(x, pltpu.VMEM)


def picks(index):
    grid = lax.broadcasted_iota(jnp.int32, (H, 1024), 0)
    hit = grid == jnp.abs(index)
    even = jnp.where(hit, 1.0, 0.0).astype(BF16)
    odd = jnp.where(hit, jnp.where(index < 0, -1.0, 1.0), 0.0).astype(BF16)
    return jnp.concatenate([even, even], axis=0), jnp.concatenate([odd, odd], axis=0)


def place(axes):
    return lax.axis_index(axes)


def plane_kernel(pot_ref, mill_ref, pos_ref, hi_ref, lo_ref, out_ref, wave_ref, cos_ref, sin_ref, *scratch):
    pot, mill, pos, hi, lo, chosen, turned, sems = scratch
    loads = [
        pltpu.make_async_copy(mill_ref, mill, sems.at[0]),
        pltpu.make_async_copy(pos_ref, pos, sems.at[1]),
        pltpu.make_async_copy(hi_ref, hi, sems.at[2]),
        pltpu.make_async_copy(lo_ref, lo, sems.at[3]),
    ]
    chunks = [
        pltpu.make_async_copy(pot_ref.at[:, pl.ds(8 * q, 8), pl.ds(h * H, H)], pot.at[q, h], sems.at[4 + 2 * q + h])
        for q in range(4)
        for h in range(2)
    ]
    for load in loads + chunks:
        load.start()
    grp = place(GRP)
    fft = place(FFT)
    loads[0].wait()
    even_x, odd_x = picks(mill[0:1, :])
    even_y, odd_y = picks(mill[1:2, :])
    loads[1].wait()
    cols = jnp.concatenate([pos[...].astype(F32), jnp.zeros((125, 128), F32)], axis=0).T
    block = pl.multiple_of((fft >> 3) * 128, 128)
    shift = (128 - (fft & 7) * 16) & 127
    near_mill = jnp.concatenate([mill[:, pl.ds(block, 128)].astype(F32), jnp.zeros((6, 128), F32)], axis=0)
    mine = pltpu.roll(near_mill, shift, 1)
    k = (cols[:, 0:1] * mine[0:1, :] + cols[:, 1:2] * mine[1:2, :]).astype(jnp.int32)
    cos_ref[...], sin_ref[...] = turn_of(jnp.bitwise_and(k, N - 1))
    zcol = cols[:, 2:3].astype(jnp.int32)
    grid = lax.broadcasted_iota(jnp.int32, (128, N), 1)
    pick = jnp.where(grid == zcol, 1.0, 0.0).astype(BF16)
    sign = 1.0 - 2.0 * jnp.bitwise_and(zcol, 1).astype(F32)
    loads[2].wait()
    loads[3].wait()
    wave = dot(pick, hi[...]) + dot(pick, lo[...])
    turn = wave * sign
    wave_ref[:, 0:H] = turn[:, :H]
    wave_ref[:, H:N] = wave[:, :H]
    wave_ref[:, N : N + H] = turn[:, H:]
    wave_ref[:, N + H :] = wave[:, H:]

    start = pl.multiple_of(grp * 32, 32)
    near_hi = hi[pl.ds(start, 32), :]
    near_lo = lo[pl.ds(start, 32), :]
    cos_y = dot(jnp.concatenate([near_hi[:, :H], near_lo[:, :H]], axis=1), even_y)
    sin_y = dot(jnp.concatenate([near_hi[:, H:], near_lo[:, H:]], axis=1), odd_y)
    wide = jnp.concatenate([hi[...], lo[...], hi[...]], axis=0)
    for q in range(4):
        halves = []
        for h in range(2):
            chunks[2 * q + h].wait()
            rows = pot.at[q, h].reshape(128, H)
            halves.append(jnp.concatenate([rows[pl.ds(y, 16, 8), :] for y in range(8)], axis=0))
        x = jnp.concatenate(halves, axis=1)
        p_hi, p_lo = split_value(x)
        w_hi, w_lo = split_value(dot(jnp.concatenate([p_hi, p_hi, p_lo], axis=1), wide))
        at = q * 128
        chosen[0, at : at + 128, 0:H] = w_hi[:, :H]
        chosen[0, at : at + 128, H:N] = w_lo[:, :H]
        chosen[1, at : at + 128, 0:H] = w_hi[:, H:]
        chosen[1, at : at + 128, H:N] = w_lo[:, H:]
    for b in range(4):
        at = b * N
        even = dot(chosen[0], even_x[:, at : at + N])
        odd = dot(chosen[1], odd_x[:, at : at + N])
        real = jnp.zeros((16, N), F32)
        imag = jnp.zeros((16, N), F32)
        for y in range(32):
            e = even[y * 16 : (y + 1) * 16, :]
            o = odd[y * 16 : (y + 1) * 16, :]
            cy = cos_y[y : y + 1, at : at + N]
            sy = sin_y[y : y + 1, at : at + N]
            real = real + (e * cy - o * sy)
            imag = imag - (e * sy + o * cy)
        for h in range(2):
            part = jnp.concatenate([real[:, h * H : (h + 1) * H], imag[:, h * H : (h + 1) * H]], axis=0)
            turned[at + h * H : at + (h + 1) * H, :] = jnp.concatenate([part] * 4, axis=0).T
    lane = lax.broadcasted_iota(jnp.int32, (16, 128), 1)
    for y in range(4):
        for x in range(4):
            base = y * 256 + x * 4
            parts = [turned[pl.ds(base + j, 16, 16), :] for j in range(4)]
            low = jnp.where(lane < 32, parts[0], parts[1])
            high = jnp.where(lane < 96, parts[2], parts[3])
            at = (y * 4 + x) * 16
            out_ref[at : at + 16, :] = jnp.where(lane < 64, low, high)


def plane_part(potential, stick_mill, positions, hi, lo):
    return pl.pallas_call(
        plane_kernel,
        out_shape=(
            pltpu.VMEM((256, 128), F32),
            pltpu.VMEM((128, 2 * N), F32),
            pltpu.VMEM((128, 128), F32),
            pltpu.VMEM((128, 128), F32),
        ),
        in_specs=[pl.BlockSpec(memory_space=pl.ANY)] * 5,
        out_specs=(VMEM,) * 4,
        scratch_shapes=[
            pltpu.VMEM((4, 2, 16, 8, H), F32),
            pltpu.VMEM((2, 1024), jnp.int32),
            pltpu.VMEM((3, 128), jnp.int32),
            pltpu.VMEM((N, N), BF16),
            pltpu.VMEM((N, N), BF16),
            pltpu.VMEM((2, 512, N), BF16),
            pltpu.VMEM((1024, 128), F32),
            pltpu.SemaphoreType.DMA((12,)),
        ],
        name="plane_part",
    )(potential, stick_mill, positions, hi, lo)


def fold_kernel(in_ref, out_ref):
    for y in range(4):
        at = y * 64
        total = (in_ref[at : at + 16, :] + in_ref[at + 16 : at + 32, :]) + (
            in_ref[at + 32 : at + 48, :] + in_ref[at + 48 : at + 64, :]
        )
        total = pltpu.roll(total, 16 - FIRST, 0)
        for core in range(2):
            out_ref[pl.ds(core * 4 + y, 16, 8), :] = total


def folded(arrived):
    return pl.pallas_call(
        fold_kernel,
        out_shape=pltpu.VMEM((128, 128), F32),
        in_specs=[VMEM],
        out_specs=VMEM,
        name="fold",
    )(near(arrived))


def line_kernel(in_ref, hi_ref, lo_ref, out_ref, turned):
    rows = [in_ref[pl.ds(y, 16, 8), :] + in_ref[pl.ds(y + 4, 16, 8), :] for y in range(4)]
    turned[...] = jnp.concatenate(rows + rows, axis=0).T
    lower = lax.broadcasted_iota(jnp.int32, (32, 128), 1) < 64
    halves = [jnp.where(lower, turned[pl.ds(2 * b, 32, 4), :], turned[pl.ds(2 * b + 1, 32, 4), :]) for b in range(2)]
    a_hi, a_lo = split_value(jnp.concatenate(halves, axis=1))
    hi = hi_ref[...]
    r = dot(a_hi, hi) + dot(a_hi, lo_ref[...]) + dot(a_lo, hi)
    first = lax.broadcasted_iota(jnp.int32, (8, N), 0) < 4
    for j in range(4):
        own = r[j * 8 : j * 8 + 8, :N]
        other = pltpu.roll(r[j * 8 : j * 8 + 8, N:], 4, 0)
        v = own + jnp.where(first, other, -other)
        for x in range(4):
            out_ref[x, j * 8 : j * 8 + 8, :] = v


def line_part(arrived, hi, lo):
    return pl.pallas_call(
        line_kernel,
        out_shape=pltpu.VMEM((4, 32, N), F32),
        in_specs=[VMEM] * 3,
        out_specs=VMEM,
        scratch_shapes=[pltpu.VMEM((128, 128), F32)],
        name="line_part",
    )(near(arrived), near(hi), near(lo))


def charge_kernel(v_ref, q_ref, wave_ref, ca_ref, sa_ref, vg_out, d_ref, mixed, vg_ref, sem):
    for s in range(16):
        top = s * 8
        for c in range(4):
            vg_ref[c, 0, s : s + 1, :] = v_ref[top + c : top + c + 1, :]
            vg_ref[c, 1, s : s + 1, :] = v_ref[top + 4 + c : top + 5 + c, :]
    save = pltpu.make_async_copy(vg_ref, vg_out, sem)
    save.start()
    for s in range(16):
        top = s * 8
        for a in range(0, 128, 16):
            ca = ca_ref[a : a + 16, s : s + 1]
            sa = sa_ref[a : a + 16, s : s + 1]
            cb = wave_ref[a : a + 16, :N]
            sb = wave_ref[a : a + 16, N:]
            cosine = ca * cb - sa * sb
            sine = sa * cb + ca * sb
            for c in range(4):
                real = v_ref[top + c : top + c + 1, :]
                imag = v_ref[top + 4 + c : top + 5 + c, :]
                mixed[c * 128 + a : c * 128 + a + 16, s * N : (s + 1) * N] = (real * cosine - imag * sine).astype(BF16)
    d = lax.dot_general(q_ref[...], mixed[...], (((1,), (1,)), ((), ())), preferred_element_type=F32)
    for c in range(4):
        d_ref[pl.ds(c, 171, 4), :] = d[:, c * 128 : (c + 1) * 128]
    d_ref[684:704, :] = jnp.zeros((20, 128), F32)
    save.wait()


def charge_part(v, charge, wave, ca, sa):
    return pl.pallas_call(
        charge_kernel,
        out_shape=(jax.ShapeDtypeStruct((4, 2, 16, N), F32), pltpu.VMEM((704, 128), F32)),
        in_specs=[VMEM] * 5,
        out_specs=(pl.BlockSpec(memory_space=pl.ANY), VMEM),
        scratch_shapes=[
            pltpu.VMEM((512, 4096), BF16),
            pltpu.VMEM((4, 2, 16, N), F32),
            pltpu.SemaphoreType.DMA(()),
        ],
        name="charge_part",
    )(near(v), near(charge), near(wave), near(ca), near(sa))


def meet_kernel(in_ref, out_ref, half):
    total = in_ref[0:88, :]
    for m in range(1, 8):
        total = total + in_ref[m * 88 : (m + 1) * 88, :]
    half[...] = total
    own = half[0:44, :] + half[44:88, :]
    for m in range(4):
        out_ref[m * 44 : (m + 1) * 44, :] = own


def met(arrived):
    return pl.pallas_call(
        meet_kernel,
        out_shape=pltpu.VMEM((176, 128), F32),
        in_specs=[VMEM],
        out_specs=VMEM,
        scratch_shapes=[pltpu.VMEM((88, 128), F32)],
        name="meet",
    )(near(arrived))


def total_kernel(in_ref, out_ref, half):
    half[...] = in_ref[0:88, :] + in_ref[88:176, :]
    own = half[0:44, :] + half[44:88, :]
    half[0:44, :] = own
    half[44:88, :] = own
    pair = half[...]
    for m in range(8):
        out_ref[m * 88 : (m + 1) * 88, :] = pair


def totals(arrived):
    return pl.pallas_call(
        total_kernel,
        out_shape=pltpu.VMEM((704, 128), F32),
        in_specs=[VMEM],
        out_specs=VMEM,
        scratch_shapes=[pltpu.VMEM((88, 128), F32)],
        name="totals",
    )(near(arrived))


def exchange(parts, axes, groups=None):
    return lax.all_to_all(parts, axes, split_axis=0, concat_axis=0, tiled=True, axis_index_groups=groups)


def body(potential, stick_mill, positions, aug_charge):
    (hi, lo), (line_hi, line_lo) = tables()
    hi, lo, line_hi, line_lo = map(jnp.asarray, (hi, lo, line_hi, line_lo))
    part, wave, ca, sa = plane_part(potential.reshape(16, 32, N), stick_mill, positions, hi, lo)
    arrived = exchange(part.reshape(16, 16, 128), ("y", "x"))
    lines = folded(arrived.reshape(256, 128))
    arrived = exchange(lines.reshape(32, 1, 512), ("zh", "zl", "core"), [LINE])
    copies = line_part(arrived.reshape(128, 128), line_hi, line_lo)
    v = exchange(copies, "x").reshape(128, N)
    v, aug_charge = lax.optimization_barrier((v, aug_charge))
    charge = aug_charge.reshape(171, 16 * N)
    vg, part = charge_part(v, charge, wave, ca, sa)
    arrived = exchange(part.reshape(16, 1, 5632), FFT, NEAR)
    mid = met(arrived.reshape(704, 128))
    arrived = exchange(mid.reshape(4, 1, 5632), FFT, CROSS)
    own = totals(arrived.reshape(176, 128))
    whole = exchange(own.reshape(16, 1, 5632), FFT, NEAR)
    return vg, jnp.moveaxis(whole.reshape(176, 4, 128)[:171], 1, 0)


def solution(mesh):
    fine = Mesh(mesh.devices.reshape(4, 4, 4, 4, 2), ("y", "zh", "zl", "x", "core"))
    placed = (P(None, FFT, GRP, None), P(), P(None, GRP), P(None, FFT, None))
    return jax.shard_map(
        body,
        mesh=fine,
        in_specs=placed,
        out_specs=(P(None, None, FFT, None), P(None, None, GRP)),
        check_vma=False,
    )
```

```python
import math

import jax
import jax.numpy as jnp
import numpy as np
from jax import lax
from jax.experimental import pallas as pl
from jax.experimental.pallas import tpu as pltpu
from jax.sharding import Mesh
from jax.sharding import PartitionSpec as P

N = 256
H = 128
GRP = ("x", "core")
FFT = ("y", "zh", "zl")
F32 = jnp.float32
BF16 = jnp.bfloat16
VMEM = pl.BlockSpec(memory_space=pltpu.VMEM)

FIRST = 10
LINE = [2 * ((FIRST + i) % 16) + core for i in range(16) for core in (1, 0)]
FAR = [[2, 7, 9, 13], [3, 6, 8, 14], [1, 5, 10, 15], [0, 4, 11, 12]]
LEADS = [9, 3, 10, 0]
NEAR = [[16 * y + four[b] for four in FAR for y in range(4)] for b in range(4)]
CROSS = [[16 * y + z for z in [lead] + [z for z in four if z != lead]] for four, lead in zip(FAR, LEADS) for y in range(4)]


def split_table(table):
    high = table.astype(np.float32).astype(jnp.bfloat16)
    low = (table - high.astype(np.float64)).astype(np.float32).astype(jnp.bfloat16)
    return high, low


def wave_table(left, right):
    angle = 2.0 * math.pi / N * np.mod(np.outer(left, right), N)
    return np.concatenate([np.cos(angle), np.sin(angle)], axis=1)


def tables():
    index = np.arange(N)
    flat = split_table(wave_table(index, index[:H]))
    z4, f = np.meshgrid(np.arange(4), np.arange(64), indexing="ij")
    f = f // 16 * 16 + (f + FIRST) % 16
    plane = (f * 4 + z4).reshape(-1)
    line = split_table(wave_table(plane, index - N // 2) * float(N) ** -1.5)
    return flat, line


def split_value(x):
    high = x.astype(BF16)
    return high, (x - high.astype(F32)).astype(BF16)


def dot(a, b):
    return jnp.dot(a, b, preferred_element_type=F32)


def fitted(values, degree=8):
    fit = np.polynomial.chebyshev.Chebyshev.interpolate(lambda w: values(np.sqrt(w)), degree, domain=[0.0, 1.0])
    return [float(c) for c in fit.convert(kind=np.polynomial.Polynomial).coef]


def turn_of(k):
    u = (k - H).astype(F32) * (1.0 / H)
    w = u * u
    even = fitted(lambda r: -np.cos(math.pi * r))
    odd = fitted(lambda r: -math.pi * np.sinc(r))
    cosine = jnp.full_like(u, even[-1])
    sine = jnp.full_like(u, odd[-1])
    for e, o in zip(even[-2::-1], odd[-2::-1]):
        cosine = cosine * w + e
        sine = sine * w + o
    return cosine, sine * u


def near(x):
    return pltpu.with_memory_space_constraint(x, pltpu.VMEM)


def picks(index):
    grid = lax.broadcasted_iota(jnp.int32, (H, 1024), 0)
    hit = grid == jnp.abs(index)
    even = jnp.where(hit, 1.0, 0.0).astype(BF16)
    odd = jnp.where(hit, jnp.where(index < 0, -1.0, 1.0), 0.0).astype(BF16)
    return jnp.concatenate([even, even], axis=0), jnp.concatenate([odd, odd], axis=0)


def place(axes):
    return lax.axis_index(axes)


def plane_kernel(pot_ref, mill_ref, pos_ref, hi_ref, lo_ref, out_ref, wave_ref, cos_ref, sin_ref, *scratch):
    pot, mill, pos, hi, lo, chosen, turned, sems = scratch
    loads = [
        pltpu.make_async_copy(mill_ref, mill, sems.at[0]),
        pltpu.make_async_copy(pos_ref, pos, sems.at[1]),
        pltpu.make_async_copy(hi_ref, hi, sems.at[2]),
        pltpu.make_async_copy(lo_ref, lo, sems.at[3]),
    ]
    chunks = [
        pltpu.make_async_copy(pot_ref.at[:, pl.ds(8 * q, 8), pl.ds(h * H, H)], pot.at[q, h], sems.at[4 + 2 * q + h])
        for q in range(4)
        for h in range(2)
    ]
    for load in loads + chunks:
        load.start()
    grp = place(GRP)
    fft = place(FFT)
    loads[0].wait()
    even_x, odd_x = picks(mill[0:1, :])
    even_y, odd_y = picks(mill[1:2, :])
    loads[1].wait()
    cols = jnp.concatenate([pos[...].astype(F32), jnp.zeros((125, 128), F32)], axis=0).T
    block = pl.multiple_of((fft >> 3) * 128, 128)
    shift = (128 - (fft & 7) * 16) & 127
    near_mill = jnp.concatenate([mill[:, pl.ds(block, 128)].astype(F32), jnp.zeros((6, 128), F32)], axis=0)
    mine = pltpu.roll(near_mill, shift, 1)
    k = (cols[:, 0:1] * mine[0:1, :] + cols[:, 1:2] * mine[1:2, :]).astype(jnp.int32)
    cos_ref[...], sin_ref[...] = turn_of(jnp.bitwise_and(k, N - 1))
    zcol = cols[:, 2:3].astype(jnp.int32)
    grid = lax.broadcasted_iota(jnp.int32, (128, N), 1)
    pick = jnp.where(grid == zcol, 1.0, 0.0).astype(BF16)
    sign = 1.0 - 2.0 * jnp.bitwise_and(zcol, 1).astype(F32)
    loads[2].wait()
    loads[3].wait()
    wave = dot(pick, hi[...]) + dot(pick, lo[...])
    turn = wave * sign
    wave_ref[:, 0:H] = turn[:, :H]
    wave_ref[:, H:N] = wave[:, :H]
    wave_ref[:, N : N + H] = turn[:, H:]
    wave_ref[:, N + H :] = wave[:, H:]

    start = pl.multiple_of(grp * 32, 32)
    near_hi = hi[pl.ds(start, 32), :]
    near_lo = lo[pl.ds(start, 32), :]
    cos_y = dot(jnp.concatenate([near_hi[:, :H], near_lo[:, :H]], axis=1), even_y)
    sin_y = dot(jnp.concatenate([near_hi[:, H:], near_lo[:, H:]], axis=1), odd_y)
    wide = jnp.concatenate([hi[...], lo[...], hi[...]], axis=0)
    for q in range(4):
        halves = []
        for h in range(2):
            chunks[2 * q + h].wait()
            rows = pot.at[q, h].reshape(128, H)
            halves.append(jnp.concatenate([rows[pl.ds(y, 16, 8), :] for y in range(8)], axis=0))
        x = jnp.concatenate(halves, axis=1)
        p_hi, p_lo = split_value(x)
        w_hi, w_lo = split_value(dot(jnp.concatenate([p_hi, p_hi, p_lo], axis=1), wide))
        at = q * 128
        chosen[0, at : at + 128, 0:H] = w_hi[:, :H]
        chosen[0, at : at + 128, H:N] = w_lo[:, :H]
        chosen[1, at : at + 128, 0:H] = w_hi[:, H:]
        chosen[1, at : at + 128, H:N] = w_lo[:, H:]
    for b in range(4):
        at = b * N
        even = dot(chosen[0], even_x[:, at : at + N])
        odd = dot(chosen[1], odd_x[:, at : at + N])
        real = jnp.zeros((16, N), F32)
        imag = jnp.zeros((16, N), F32)
        for y in range(32):
            e = even[y * 16 : (y + 1) * 16, :]
            o = odd[y * 16 : (y + 1) * 16, :]
            cy = cos_y[y : y + 1, at : at + N]
            sy = sin_y[y : y + 1, at : at + N]
            real = real + (e * cy - o * sy)
            imag = imag - (e * sy + o * cy)
        for h in range(2):
            part = jnp.concatenate([real[:, h * H : (h + 1) * H], imag[:, h * H : (h + 1) * H]], axis=0)
            turned[at + h * H : at + (h + 1) * H, :] = jnp.concatenate([part] * 4, axis=0).T
    lane = lax.broadcasted_iota(jnp.int32, (16, 128), 1)
    for y in range(4):
        for x in range(4):
            base = y * 256 + x * 4
            parts = [turned[pl.ds(base + j, 16, 16), :] for j in range(4)]
            low = jnp.where(lane < 32, parts[0], parts[1])
            high = jnp.where(lane < 96, parts[2], parts[3])
            at = (y * 4 + x) * 16
            out_ref[at : at + 16, :] = jnp.where(lane < 64, low, high)


def plane_part(potential, stick_mill, positions, hi, lo):
    return pl.pallas_call(
        plane_kernel,
        out_shape=(
            pltpu.VMEM((256, 128), F32),
            pltpu.VMEM((128, 2 * N), F32),
            pltpu.VMEM((128, 128), F32),
            pltpu.VMEM((128, 128), F32),
        ),
        in_specs=[pl.BlockSpec(memory_space=pl.ANY)] * 5,
        out_specs=(VMEM,) * 4,
        scratch_shapes=[
            pltpu.VMEM((4, 2, 16, 8, H), F32),
            pltpu.VMEM((2, 1024), jnp.int32),
            pltpu.VMEM((3, 128), jnp.int32),
            pltpu.VMEM((N, N), BF16),
            pltpu.VMEM((N, N), BF16),
            pltpu.VMEM((2, 512, N), BF16),
            pltpu.VMEM((1024, 128), F32),
            pltpu.SemaphoreType.DMA((12,)),
        ],
        name="plane_part",
    )(potential, stick_mill, positions, hi, lo)


def fold_kernel(in_ref, out_ref):
    for y in range(4):
        at = y * 64
        total = (in_ref[at : at + 16, :] + in_ref[at + 16 : at + 32, :]) + (
            in_ref[at + 32 : at + 48, :] + in_ref[at + 48 : at + 64, :]
        )
        total = pltpu.roll(total, 16 - FIRST, 0)
        for core in range(2):
            out_ref[pl.ds(core * 4 + y, 16, 8), :] = total


def folded(arrived):
    return pl.pallas_call(
        fold_kernel,
        out_shape=pltpu.VMEM((128, 128), F32),
        in_specs=[VMEM],
        out_specs=VMEM,
        name="fold",
    )(near(arrived))


def line_kernel(in_ref, hi_ref, lo_ref, out_ref, turned):
    rows = [in_ref[pl.ds(y, 16, 8), :] + in_ref[pl.ds(y + 4, 16, 8), :] for y in range(4)]
    turned[...] = jnp.concatenate(rows + rows, axis=0).T
    lower = lax.broadcasted_iota(jnp.int32, (32, 128), 1) < 64
    halves = [jnp.where(lower, turned[pl.ds(2 * b, 32, 4), :], turned[pl.ds(2 * b + 1, 32, 4), :]) for b in range(2)]
    a_hi, a_lo = split_value(jnp.concatenate(halves, axis=1))
    hi = hi_ref[...]
    r = dot(a_hi, hi) + dot(a_hi, lo_ref[...]) + dot(a_lo, hi)
    first = lax.broadcasted_iota(jnp.int32, (8, N), 0) < 4
    for j in range(4):
        own = r[j * 8 : j * 8 + 8, :N]
        other = pltpu.roll(r[j * 8 : j * 8 + 8, N:], 4, 0)
        v = own + jnp.where(first, other, -other)
        for x in range(4):
            out_ref[x, j * 8 : j * 8 + 8, :] = v


def line_part(arrived, hi, lo):
    return pl.pallas_call(
        line_kernel,
        out_shape=pltpu.VMEM((4, 32, N), F32),
        in_specs=[VMEM] * 3,
        out_specs=VMEM,
        scratch_shapes=[pltpu.VMEM((128, 128), F32)],
        name="line_part",
    )(near(arrived), near(hi), near(lo))


def charge_kernel(v_ref, q_ref, wave_ref, ca_ref, sa_ref, vg_out, d_ref, mixed, vg_ref, sem):
    for s in range(16):
        top = s * 8
        for c in range(4):
            vg_ref[c, 0, s : s + 1, :] = v_ref[top + c : top + c + 1, :]
            vg_ref[c, 1, s : s + 1, :] = v_ref[top + 4 + c : top + 5 + c, :]
    save = pltpu.make_async_copy(vg_ref, vg_out, sem)
    save.start()
    for s in range(16):
        top = s * 8
        for a in range(0, 128, 16):
            ca = ca_ref[a : a + 16, s : s + 1]
            sa = sa_ref[a : a + 16, s : s + 1]
            cb = wave_ref[a : a + 16, :N]
            sb = wave_ref[a : a + 16, N:]
            cosine = ca * cb - sa * sb
            sine = sa * cb + ca * sb
            for c in range(4):
                real = v_ref[top + c : top + c + 1, :]
                imag = v_ref[top + 4 + c : top + 5 + c, :]
                mixed[c * 128 + a : c * 128 + a + 16, s * N : (s + 1) * N] = (real * cosine - imag * sine).astype(BF16)
    d = lax.dot_general(q_ref[...], mixed[...], (((1,), (1,)), ((), ())), preferred_element_type=F32)
    for c in range(4):
        d_ref[pl.ds(c, 171, 4), :] = d[:, c * 128 : (c + 1) * 128]
    d_ref[684:704, :] = jnp.zeros((20, 128), F32)
    save.wait()


def charge_part(v, charge, wave, ca, sa):
    return pl.pallas_call(
        charge_kernel,
        out_shape=(jax.ShapeDtypeStruct((4, 2, 16, N), F32), pltpu.VMEM((704, 128), F32)),
        in_specs=[VMEM] * 5,
        out_specs=(pl.BlockSpec(memory_space=pl.ANY), VMEM),
        scratch_shapes=[
            pltpu.VMEM((512, 4096), BF16),
            pltpu.VMEM((4, 2, 16, N), F32),
            pltpu.SemaphoreType.DMA(()),
        ],
        name="charge_part",
    )(near(v), near(charge), near(wave), near(ca), near(sa))


def meet_kernel(in_ref, out_ref, half):
    total = in_ref[0:88, :]
    for m in range(1, 8):
        total = total + in_ref[m * 88 : (m + 1) * 88, :]
    half[...] = total
    own = half[0:44, :] + half[44:88, :]
    for m in range(4):
        out_ref[m * 44 : (m + 1) * 44, :] = own


def met(arrived):
    return pl.pallas_call(
        meet_kernel,
        out_shape=pltpu.VMEM((176, 128), F32),
        in_specs=[VMEM],
        out_specs=VMEM,
        scratch_shapes=[pltpu.VMEM((88, 128), F32)],
        name="meet",
    )(near(arrived))


def total_kernel(in_ref, out_ref, half):
    half[...] = in_ref[0:88, :] + in_ref[88:176, :]
    own = half[0:44, :] + half[44:88, :]
    half[0:44, :] = own
    half[44:88, :] = own
    pair = half[...]
    for m in range(8):
        out_ref[m * 88 : (m + 1) * 88, :] = pair


def totals(arrived):
    return pl.pallas_call(
        total_kernel,
        out_shape=pltpu.VMEM((704, 128), F32),
        in_specs=[VMEM],
        out_specs=VMEM,
        scratch_shapes=[pltpu.VMEM((88, 128), F32)],
        name="totals",
    )(near(arrived))


def save_kernel(in_ref, out_ref, sem):
    save = pltpu.make_async_copy(in_ref.at[pl.ds(0, 171)], out_ref, sem)
    save.start()
    save.wait()


def saved(whole):
    return pl.pallas_call(
        save_kernel,
        out_shape=jax.ShapeDtypeStruct((171, 4, 128), F32),
        in_specs=[VMEM],
        out_specs=pl.BlockSpec(memory_space=pl.ANY),
        scratch_shapes=[pltpu.SemaphoreType.DMA(())],
        name="saved",
    )(near(whole))


def exchange(parts, axes, groups=None):
    return lax.all_to_all(parts, axes, split_axis=0, concat_axis=0, tiled=True, axis_index_groups=groups)


def body(potential, stick_mill, positions, aug_charge):
    (hi, lo), (line_hi, line_lo) = tables()
    hi, lo, line_hi, line_lo = map(jnp.asarray, (hi, lo, line_hi, line_lo))
    part, wave, ca, sa = plane_part(potential.reshape(16, 32, N), stick_mill, positions, hi, lo)
    arrived = exchange(part.reshape(16, 16, 128), ("y", "x"))
    lines = folded(arrived.reshape(256, 128))
    arrived = exchange(lines.reshape(32, 1, 512), ("zh", "zl", "core"), [LINE])
    copies = line_part(arrived.reshape(128, 128), line_hi, line_lo)
    v = exchange(copies, "x").reshape(128, N)
    v, aug_charge = lax.optimization_barrier((v, aug_charge))
    charge = aug_charge.reshape(171, 16 * N)
    vg, part = charge_part(v, charge, wave, ca, sa)
    arrived = exchange(part.reshape(16, 1, 5632), FFT, NEAR)
    mid = met(arrived.reshape(704, 128))
    arrived = exchange(mid.reshape(4, 1, 5632), FFT, CROSS)
    own = totals(arrived.reshape(176, 128))
    whole = exchange(own.reshape(16, 1, 5632), FFT, NEAR)
    return vg, jnp.moveaxis(saved(whole.reshape(176, 4, 128)), 1, 0)


def solution(mesh):
    fine = Mesh(mesh.devices.reshape(4, 4, 4, 4, 2), ("y", "zh", "zl", "x", "core"))
    placed = (P(None, FFT, GRP, None), P(), P(None, GRP), P(None, FFT, None))
    return jax.shard_map(
        body,
        mesh=fine,
        in_specs=placed,
        out_specs=(P(None, None, FFT, None), P(None, None, GRP)),
        check_vma=False,
    )
```

```python
import math

import jax
import jax.numpy as jnp
import numpy as np
from jax import lax
from jax.experimental import pallas as pl
from jax.experimental.pallas import tpu as pltpu
from jax.sharding import Mesh
from jax.sharding import PartitionSpec as P

N = 256
H = 128
GRP = ("x", "core")
FFT = ("y", "zh", "zl")
F32 = jnp.float32
BF16 = jnp.bfloat16
VMEM = pl.BlockSpec(memory_space=pltpu.VMEM)

FIRST = 10
LINE = [2 * ((FIRST + i) % 16) + core for i in range(16) for core in (1, 0)]
FAR = [[2, 6, 9, 13], [0, 4, 10, 14], [1, 5, 11, 15], [3, 7, 8, 12]]
LEADS = [9, 10, 11, 8]
NEAR = [[16 * y + four[b] for four in FAR for y in range(4)] for b in range(4)]
CROSS = [[16 * y + z for z in [lead] + [z for z in four if z != lead]] for four, lead in zip(FAR, LEADS) for y in range(4)]


def split_table(table):
    high = table.astype(np.float32).astype(jnp.bfloat16)
    low = (table - high.astype(np.float64)).astype(np.float32).astype(jnp.bfloat16)
    return high, low


def wave_table(left, right):
    angle = 2.0 * math.pi / N * np.mod(np.outer(left, right), N)
    return np.concatenate([np.cos(angle), np.sin(angle)], axis=1)


def tables():
    index = np.arange(N)
    flat = split_table(wave_table(index, index[:H]))
    z4, f = np.meshgrid(np.arange(4), np.arange(64), indexing="ij")
    f = f // 16 * 16 + (f + FIRST) % 16
    plane = (f * 4 + z4).reshape(-1)
    line = split_table(wave_table(plane, index - N // 2) * float(N) ** -1.5)
    return flat, line


def split_value(x):
    high = x.astype(BF16)
    return high, (x - high.astype(F32)).astype(BF16)


def dot(a, b):
    return jnp.dot(a, b, preferred_element_type=F32)


def fitted(values, degree=8):
    fit = np.polynomial.chebyshev.Chebyshev.interpolate(lambda w: values(np.sqrt(w)), degree, domain=[0.0, 1.0])
    return [float(c) for c in fit.convert(kind=np.polynomial.Polynomial).coef]


def turn_of(k):
    u = (k - H).astype(F32) * (1.0 / H)
    w = u * u
    even = fitted(lambda r: -np.cos(math.pi * r))
    odd = fitted(lambda r: -math.pi * np.sinc(r))
    cosine = jnp.full_like(u, even[-1])
    sine = jnp.full_like(u, odd[-1])
    for e, o in zip(even[-2::-1], odd[-2::-1]):
        cosine = cosine * w + e
        sine = sine * w + o
    return cosine, sine * u


def near(x):
    return pltpu.with_memory_space_constraint(x, pltpu.VMEM)


def picks(index):
    grid = lax.broadcasted_iota(jnp.int32, (H, 1024), 0)
    hit = grid == jnp.abs(index)
    even = jnp.where(hit, 1.0, 0.0).astype(BF16)
    odd = jnp.where(hit, jnp.where(index < 0, -1.0, 1.0), 0.0).astype(BF16)
    return jnp.concatenate([even, even], axis=0), jnp.concatenate([odd, odd], axis=0)


def place(axes):
    return lax.axis_index(axes)


def plane_kernel(pot_ref, mill_ref, pos_ref, hi_ref, lo_ref, out_ref, wave_ref, cos_ref, sin_ref, *scratch):
    pot, mill, pos, hi, lo, chosen, turned, sems = scratch
    loads = [
        pltpu.make_async_copy(mill_ref, mill, sems.at[0]),
        pltpu.make_async_copy(pos_ref, pos, sems.at[1]),
        pltpu.make_async_copy(hi_ref, hi, sems.at[2]),
        pltpu.make_async_copy(lo_ref, lo, sems.at[3]),
    ]
    chunks = [
        pltpu.make_async_copy(pot_ref.at[:, pl.ds(8 * q, 8), pl.ds(h * H, H)], pot.at[q, h], sems.at[4 + 2 * q + h])
        for q in range(4)
        for h in range(2)
    ]
    for load in loads + chunks:
        load.start()
    grp = place(GRP)
    fft = place(FFT)
    loads[0].wait()
    even_x, odd_x = picks(mill[0:1, :])
    even_y, odd_y = picks(mill[1:2, :])
    loads[1].wait()
    cols = jnp.concatenate([pos[...].astype(F32), jnp.zeros((125, 128), F32)], axis=0).T
    block = pl.multiple_of((fft >> 3) * 128, 128)
    shift = (128 - (fft & 7) * 16) & 127
    near_mill = jnp.concatenate([mill[:, pl.ds(block, 128)].astype(F32), jnp.zeros((6, 128), F32)], axis=0)
    mine = pltpu.roll(near_mill, shift, 1)
    k = (cols[:, 0:1] * mine[0:1, :] + cols[:, 1:2] * mine[1:2, :]).astype(jnp.int32)
    cos_ref[...], sin_ref[...] = turn_of(jnp.bitwise_and(k, N - 1))
    zcol = cols[:, 2:3].astype(jnp.int32)
    grid = lax.broadcasted_iota(jnp.int32, (128, N), 1)
    pick = jnp.where(grid == zcol, 1.0, 0.0).astype(BF16)
    sign = 1.0 - 2.0 * jnp.bitwise_and(zcol, 1).astype(F32)
    loads[2].wait()
    loads[3].wait()
    wave = dot(pick, hi[...]) + dot(pick, lo[...])
    turn = wave * sign
    wave_ref[:, 0:H] = turn[:, :H]
    wave_ref[:, H:N] = wave[:, :H]
    wave_ref[:, N : N + H] = turn[:, H:]
    wave_ref[:, N + H :] = wave[:, H:]

    start = pl.multiple_of(grp * 32, 32)
    near_hi = hi[pl.ds(start, 32), :]
    near_lo = lo[pl.ds(start, 32), :]
    cos_y = dot(jnp.concatenate([near_hi[:, :H], near_lo[:, :H]], axis=1), even_y)
    sin_y = dot(jnp.concatenate([near_hi[:, H:], near_lo[:, H:]], axis=1), odd_y)
    wide = jnp.concatenate([hi[...], lo[...], hi[...]], axis=0)
    for q in range(4):
        halves = []
        for h in range(2):
            chunks[2 * q + h].wait()
            rows = pot.at[q, h].reshape(128, H)
            halves.append(jnp.concatenate([rows[pl.ds(y, 16, 8), :] for y in range(8)], axis=0))
        x = jnp.concatenate(halves, axis=1)
        p_hi, p_lo = split_value(x)
        w_hi, w_lo = split_value(dot(jnp.concatenate([p_hi, p_hi, p_lo], axis=1), wide))
        at = q * 128
        chosen[0, at : at + 128, 0:H] = w_hi[:, :H]
        chosen[0, at : at + 128, H:N] = w_lo[:, :H]
        chosen[1, at : at + 128, 0:H] = w_hi[:, H:]
        chosen[1, at : at + 128, H:N] = w_lo[:, H:]
    for b in range(4):
        at = b * N
        even = dot(chosen[0], even_x[:, at : at + N])
        odd = dot(chosen[1], odd_x[:, at : at + N])
        real = jnp.zeros((16, N), F32)
        imag = jnp.zeros((16, N), F32)
        for y in range(32):
            e = even[y * 16 : (y + 1) * 16, :]
            o = odd[y * 16 : (y + 1) * 16, :]
            cy = cos_y[y : y + 1, at : at + N]
            sy = sin_y[y : y + 1, at : at + N]
            real = real + (e * cy - o * sy)
            imag = imag - (e * sy + o * cy)
        for h in range(2):
            part = jnp.concatenate([real[:, h * H : (h + 1) * H], imag[:, h * H : (h + 1) * H]], axis=0)
            turned[at + h * H : at + (h + 1) * H, :] = jnp.concatenate([part] * 4, axis=0).T
    lane = lax.broadcasted_iota(jnp.int32, (16, 128), 1)
    for y in range(4):
        for x in range(4):
            base = y * 256 + x * 4
            parts = [turned[pl.ds(base + j, 16, 16), :] for j in range(4)]
            low = jnp.where(lane < 32, parts[0], parts[1])
            high = jnp.where(lane < 96, parts[2], parts[3])
            at = (y * 4 + x) * 16
            out_ref[at : at + 16, :] = jnp.where(lane < 64, low, high)


def plane_part(potential, stick_mill, positions, hi, lo):
    return pl.pallas_call(
        plane_kernel,
        out_shape=(
            pltpu.VMEM((256, 128), F32),
            pltpu.VMEM((128, 2 * N), F32),
            pltpu.VMEM((128, 128), F32),
            pltpu.VMEM((128, 128), F32),
        ),
        in_specs=[pl.BlockSpec(memory_space=pl.ANY)] * 5,
        out_specs=(VMEM,) * 4,
        scratch_shapes=[
            pltpu.VMEM((4, 2, 16, 8, H), F32),
            pltpu.VMEM((2, 1024), jnp.int32),
            pltpu.VMEM((3, 128), jnp.int32),
            pltpu.VMEM((N, N), BF16),
            pltpu.VMEM((N, N), BF16),
            pltpu.VMEM((2, 512, N), BF16),
            pltpu.VMEM((1024, 128), F32),
            pltpu.SemaphoreType.DMA((12,)),
        ],
        name="plane_part",
    )(potential, stick_mill, positions, hi, lo)


def fold_kernel(in_ref, out_ref):
    for y in range(4):
        at = y * 64
        total = (in_ref[at : at + 16, :] + in_ref[at + 16 : at + 32, :]) + (
            in_ref[at + 32 : at + 48, :] + in_ref[at + 48 : at + 64, :]
        )
        total = pltpu.roll(total, 16 - FIRST, 0)
        for core in range(2):
            out_ref[pl.ds(core * 4 + y, 16, 8), :] = total


def folded(arrived):
    return pl.pallas_call(
        fold_kernel,
        out_shape=pltpu.VMEM((128, 128), F32),
        in_specs=[VMEM],
        out_specs=VMEM,
        name="fold",
    )(near(arrived))


def line_kernel(in_ref, hi_ref, lo_ref, out_ref, turned):
    rows = [in_ref[pl.ds(y, 16, 8), :] + in_ref[pl.ds(y + 4, 16, 8), :] for y in range(4)]
    turned[...] = jnp.concatenate(rows + rows, axis=0).T
    lower = lax.broadcasted_iota(jnp.int32, (32, 128), 1) < 64
    halves = [jnp.where(lower, turned[pl.ds(2 * b, 32, 4), :], turned[pl.ds(2 * b + 1, 32, 4), :]) for b in range(2)]
    a_hi, a_lo = split_value(jnp.concatenate(halves, axis=1))
    hi = hi_ref[...]
    r = dot(a_hi, hi) + dot(a_hi, lo_ref[...]) + dot(a_lo, hi)
    first = lax.broadcasted_iota(jnp.int32, (8, N), 0) < 4
    for j in range(4):
        own = r[j * 8 : j * 8 + 8, :N]
        other = pltpu.roll(r[j * 8 : j * 8 + 8, N:], 4, 0)
        v = own + jnp.where(first, other, -other)
        for x in range(4):
            out_ref[x, j * 8 : j * 8 + 8, :] = v


def line_part(arrived, hi, lo):
    return pl.pallas_call(
        line_kernel,
        out_shape=pltpu.VMEM((4, 32, N), F32),
        in_specs=[VMEM] * 3,
        out_specs=VMEM,
        scratch_shapes=[pltpu.VMEM((128, 128), F32)],
        name="line_part",
    )(near(arrived), near(hi), near(lo))


def charge_kernel(v_ref, q_ref, wave_ref, ca_ref, sa_ref, vg_out, d_ref, mixed, vg_ref, sem):
    for s in range(16):
        top = s * 8
        for c in range(4):
            vg_ref[c, 0, s : s + 1, :] = v_ref[top + c : top + c + 1, :]
            vg_ref[c, 1, s : s + 1, :] = v_ref[top + 4 + c : top + 5 + c, :]
    save = pltpu.make_async_copy(vg_ref, vg_out, sem)
    save.start()
    for s in range(16):
        top = s * 8
        for a in range(0, 128, 16):
            ca = ca_ref[a : a + 16, s : s + 1]
            sa = sa_ref[a : a + 16, s : s + 1]
            cb = wave_ref[a : a + 16, :N]
            sb = wave_ref[a : a + 16, N:]
            cosine = ca * cb - sa * sb
            sine = sa * cb + ca * sb
            for c in range(4):
                real = v_ref[top + c : top + c + 1, :]
                imag = v_ref[top + 4 + c : top + 5 + c, :]
                mixed[c * 128 + a : c * 128 + a + 16, s * N : (s + 1) * N] = (real * cosine - imag * sine).astype(BF16)
    d = lax.dot_general(q_ref[...], mixed[...], (((1,), (1,)), ((), ())), preferred_element_type=F32)
    for c in range(4):
        d_ref[pl.ds(c, 171, 4), :] = d[:, c * 128 : (c + 1) * 128]
    d_ref[684:704, :] = jnp.zeros((20, 128), F32)
    save.wait()


def charge_part(v, charge, wave, ca, sa):
    return pl.pallas_call(
        charge_kernel,
        out_shape=(jax.ShapeDtypeStruct((4, 2, 16, N), F32), pltpu.VMEM((704, 128), F32)),
        in_specs=[VMEM] * 5,
        out_specs=(pl.BlockSpec(memory_space=pl.ANY), VMEM),
        scratch_shapes=[
            pltpu.VMEM((512, 4096), BF16),
            pltpu.VMEM((4, 2, 16, N), F32),
            pltpu.SemaphoreType.DMA(()),
        ],
        name="charge_part",
    )(near(v), near(charge), near(wave), near(ca), near(sa))


def meet_kernel(in_ref, out_ref, half):
    total = in_ref[0:88, :]
    for m in range(1, 8):
        total = total + in_ref[m * 88 : (m + 1) * 88, :]
    half[...] = total
    own = half[0:44, :] + half[44:88, :]
    for m in range(4):
        out_ref[m * 44 : (m + 1) * 44, :] = own


def met(arrived):
    return pl.pallas_call(
        meet_kernel,
        out_shape=pltpu.VMEM((176, 128), F32),
        in_specs=[VMEM],
        out_specs=VMEM,
        scratch_shapes=[pltpu.VMEM((88, 128), F32)],
        name="meet",
    )(near(arrived))


def total_kernel(in_ref, out_ref, half):
    half[...] = in_ref[0:88, :] + in_ref[88:176, :]
    own = half[0:44, :] + half[44:88, :]
    half[0:44, :] = own
    half[44:88, :] = own
    pair = half[...]
    for m in range(8):
        out_ref[m * 88 : (m + 1) * 88, :] = pair


def totals(arrived):
    return pl.pallas_call(
        total_kernel,
        out_shape=pltpu.VMEM((704, 128), F32),
        in_specs=[VMEM],
        out_specs=VMEM,
        scratch_shapes=[pltpu.VMEM((88, 128), F32)],
        name="totals",
    )(near(arrived))


def exchange(parts, axes, groups=None):
    return lax.all_to_all(parts, axes, split_axis=0, concat_axis=0, tiled=True, axis_index_groups=groups)


def body(potential, stick_mill, positions, aug_charge):
    (hi, lo), (line_hi, line_lo) = tables()
    hi, lo, line_hi, line_lo = map(jnp.asarray, (hi, lo, line_hi, line_lo))
    part, wave, ca, sa = plane_part(potential.reshape(16, 32, N), stick_mill, positions, hi, lo)
    arrived = exchange(part.reshape(16, 16, 128), ("y", "x"))
    lines = folded(arrived.reshape(256, 128))
    arrived = exchange(lines.reshape(32, 1, 512), ("zh", "zl", "core"), [LINE])
    copies = line_part(arrived.reshape(128, 128), line_hi, line_lo)
    v = exchange(copies, "x").reshape(128, N)
    v, aug_charge = lax.optimization_barrier((v, aug_charge))
    charge = aug_charge.reshape(171, 16 * N)
    vg, part = charge_part(v, charge, wave, ca, sa)
    arrived = exchange(part.reshape(16, 1, 5632), FFT, NEAR)
    mid = met(arrived.reshape(704, 128))
    arrived = exchange(mid.reshape(4, 1, 5632), FFT, CROSS)
    own = totals(arrived.reshape(176, 128))
    whole = exchange(own.reshape(16, 1, 5632), FFT, NEAR)
    return vg, jnp.moveaxis(whole.reshape(176, 4, 128)[:171], 1, 0)


def solution(mesh):
    fine = Mesh(mesh.devices.reshape(4, 4, 4, 4, 2), ("y", "zh", "zl", "x", "core"))
    placed = (P(None, FFT, GRP, None), P(), P(None, GRP), P(None, FFT, None))
    return jax.shard_map(
        body,
        mesh=fine,
        in_specs=placed,
        out_specs=(P(None, None, FFT, None), P(None, None, GRP)),
        check_vma=False,
    )
```

```python
import math

import jax
import jax.numpy as jnp
import numpy as np
from jax import lax
from jax.experimental import pallas as pl
from jax.experimental.pallas import tpu as pltpu
from jax.sharding import Mesh
from jax.sharding import PartitionSpec as P

N = 256
H = 128
GRP = ("x", "core")
FFT = ("y", "zh", "zl")
F32 = jnp.float32
BF16 = jnp.bfloat16
VMEM = pl.BlockSpec(memory_space=pltpu.VMEM)

FIRST = 10
LINE = [2 * ((FIRST + i) % 16) + core for i in range(16) for core in (1, 0)]
FAR = [[1, 6, 8, 12], [0, 5, 9, 14], [2, 4, 10, 15], [3, 7, 11, 13]]
LEADS = [8, 9, 10, 11]
TURN = [2, 3, 0, 1]
SQUARE = [4 * y + x for y in TURN for x in TURN]
NEAR = [[16 * y + four[b] for four in FAR for y in TURN] for b in range(4)]
CROSS = [[16 * y + z for z in [lead] + [z for z in four if z != lead]] for four, lead in zip(FAR, LEADS) for y in range(4)]


def split_table(table):
    high = table.astype(np.float32).astype(jnp.bfloat16)
    low = (table - high.astype(np.float64)).astype(np.float32).astype(jnp.bfloat16)
    return high, low


def wave_table(left, right):
    angle = 2.0 * math.pi / N * np.mod(np.outer(left, right), N)
    return np.concatenate([np.cos(angle), np.sin(angle)], axis=1)


def tables():
    index = np.arange(N)
    flat = split_table(wave_table(index, index[:H]))
    z4, f = np.meshgrid(np.arange(4), np.arange(64), indexing="ij")
    f = f // 16 * 16 + (f + FIRST) % 16
    plane = (f * 4 + z4).reshape(-1)
    line = split_table(wave_table(plane, index - N // 2) * float(N) ** -1.5)
    return flat, line


def split_value(x):
    high = x.astype(BF16)
    return high, (x - high.astype(F32)).astype(BF16)


def dot(a, b):
    return jnp.dot(a, b, preferred_element_type=F32)


def fitted(values, degree=8):
    fit = np.polynomial.chebyshev.Chebyshev.interpolate(lambda w: values(np.sqrt(w)), degree, domain=[0.0, 1.0])
    return [float(c) for c in fit.convert(kind=np.polynomial.Polynomial).coef]


def turn_of(k):
    u = (k - H).astype(F32) * (1.0 / H)
    w = u * u
    even = fitted(lambda r: -np.cos(math.pi * r))
    odd = fitted(lambda r: -math.pi * np.sinc(r))
    cosine = jnp.full_like(u, even[-1])
    sine = jnp.full_like(u, odd[-1])
    for e, o in zip(even[-2::-1], odd[-2::-1]):
        cosine = cosine * w + e
        sine = sine * w + o
    return cosine, sine * u


def near(x):
    return pltpu.with_memory_space_constraint(x, pltpu.VMEM)


def picks(index):
    grid = lax.broadcasted_iota(jnp.int32, (H, 1024), 0)
    hit = grid == jnp.abs(index)
    even = jnp.where(hit, 1.0, 0.0).astype(BF16)
    odd = jnp.where(hit, jnp.where(index < 0, -1.0, 1.0), 0.0).astype(BF16)
    return jnp.concatenate([even, even], axis=0), jnp.concatenate([odd, odd], axis=0)


def place(axes):
    return lax.axis_index(axes)


def plane_kernel(pot_ref, mill_ref, pos_ref, hi_ref, lo_ref, out_ref, wave_ref, cos_ref, sin_ref, *scratch):
    pot, mill, pos, hi, lo, chosen, turned, sems = scratch
    loads = [
        pltpu.make_async_copy(mill_ref, mill, sems.at[0]),
        pltpu.make_async_copy(pos_ref, pos, sems.at[1]),
        pltpu.make_async_copy(hi_ref, hi, sems.at[2]),
        pltpu.make_async_copy(lo_ref, lo, sems.at[3]),
    ]
    chunks = [
        pltpu.make_async_copy(pot_ref.at[:, pl.ds(8 * q, 8), pl.ds(h * H, H)], pot.at[q, h], sems.at[4 + 2 * q + h])
        for q in range(4)
        for h in range(2)
    ]
    for load in loads + chunks:
        load.start()
    grp = place(GRP)
    fft = place(FFT)
    loads[0].wait()
    even_x, odd_x = picks(mill[0:1, :])
    even_y, odd_y = picks(mill[1:2, :])
    loads[1].wait()
    cols = jnp.concatenate([pos[...].astype(F32), jnp.zeros((125, 128), F32)], axis=0).T
    block = pl.multiple_of((fft >> 3) * 128, 128)
    shift = (128 - (fft & 7) * 16) & 127
    near_mill = jnp.concatenate([mill[:, pl.ds(block, 128)].astype(F32), jnp.zeros((6, 128), F32)], axis=0)
    mine = pltpu.roll(near_mill, shift, 1)
    k = (cols[:, 0:1] * mine[0:1, :] + cols[:, 1:2] * mine[1:2, :]).astype(jnp.int32)
    cos_ref[...], sin_ref[...] = turn_of(jnp.bitwise_and(k, N - 1))
    zcol = cols[:, 2:3].astype(jnp.int32)
    grid = lax.broadcasted_iota(jnp.int32, (128, N), 1)
    pick = jnp.where(grid == zcol, 1.0, 0.0).astype(BF16)
    sign = 1.0 - 2.0 * jnp.bitwise_and(zcol, 1).astype(F32)
    loads[2].wait()
    loads[3].wait()
    wave = dot(pick, hi[...]) + dot(pick, lo[...])
    turn = wave * sign
    wave_ref[:, 0:H] = turn[:, :H]
    wave_ref[:, H:N] = wave[:, :H]
    wave_ref[:, N : N + H] = turn[:, H:]
    wave_ref[:, N + H :] = wave[:, H:]

    start = pl.multiple_of(grp * 32, 32)
    near_hi = hi[pl.ds(start, 32), :]
    near_lo = lo[pl.ds(start, 32), :]
    cos_y = dot(jnp.concatenate([near_hi[:, :H], near_lo[:, :H]], axis=1), even_y)
    sin_y = dot(jnp.concatenate([near_hi[:, H:], near_lo[:, H:]], axis=1), odd_y)
    wide = jnp.concatenate([hi[...], lo[...], hi[...]], axis=0)
    for q in range(4):
        halves = []
        for h in range(2):
            chunks[2 * q + h].wait()
            rows = pot.at[q, h].reshape(128, H)
            halves.append(jnp.concatenate([rows[pl.ds(y, 16, 8), :] for y in range(8)], axis=0))
        x = jnp.concatenate(halves, axis=1)
        p_hi, p_lo = split_value(x)
        w_hi, w_lo = split_value(dot(jnp.concatenate([p_hi, p_hi, p_lo], axis=1), wide))
        at = q * 128
        chosen[0, at : at + 128, 0:H] = w_hi[:, :H]
        chosen[0, at : at + 128, H:N] = w_lo[:, :H]
        chosen[1, at : at + 128, 0:H] = w_hi[:, H:]
        chosen[1, at : at + 128, H:N] = w_lo[:, H:]
    for b in range(4):
        at = b * N
        even = dot(chosen[0], even_x[:, at : at + N])
        odd = dot(chosen[1], odd_x[:, at : at + N])
        real = jnp.zeros((16, N), F32)
        imag = jnp.zeros((16, N), F32)
        for y in range(32):
            e = even[y * 16 : (y + 1) * 16, :]
            o = odd[y * 16 : (y + 1) * 16, :]
            cy = cos_y[y : y + 1, at : at + N]
            sy = sin_y[y : y + 1, at : at + N]
            real = real + (e * cy - o * sy)
            imag = imag - (e * sy + o * cy)
        for h in range(2):
            part = jnp.concatenate([real[:, h * H : (h + 1) * H], imag[:, h * H : (h + 1) * H]], axis=0)
            turned[at + h * H : at + (h + 1) * H, :] = jnp.concatenate([part] * 4, axis=0).T
    lane = lax.broadcasted_iota(jnp.int32, (16, 128), 1)
    for y in range(4):
        for x in range(4):
            base = TURN[y] * 256 + TURN[x] * 4
            parts = [turned[pl.ds(base + j, 16, 16), :] for j in range(4)]
            low = jnp.where(lane < 32, parts[0], parts[1])
            high = jnp.where(lane < 96, parts[2], parts[3])
            at = (y * 4 + x) * 16
            out_ref[at : at + 16, :] = jnp.where(lane < 64, low, high)


def plane_part(potential, stick_mill, positions, hi, lo):
    return pl.pallas_call(
        plane_kernel,
        out_shape=(
            pltpu.VMEM((256, 128), F32),
            pltpu.VMEM((128, 2 * N), F32),
            pltpu.VMEM((128, 128), F32),
            pltpu.VMEM((128, 128), F32),
        ),
        in_specs=[pl.BlockSpec(memory_space=pl.ANY)] * 5,
        out_specs=(VMEM,) * 4,
        scratch_shapes=[
            pltpu.VMEM((4, 2, 16, 8, H), F32),
            pltpu.VMEM((2, 1024), jnp.int32),
            pltpu.VMEM((3, 128), jnp.int32),
            pltpu.VMEM((N, N), BF16),
            pltpu.VMEM((N, N), BF16),
            pltpu.VMEM((2, 512, N), BF16),
            pltpu.VMEM((1024, 128), F32),
            pltpu.SemaphoreType.DMA((12,)),
        ],
        name="plane_part",
    )(potential, stick_mill, positions, hi, lo)


def fold_kernel(in_ref, out_ref):
    for y in range(4):
        at = y * 64
        total = (in_ref[at : at + 16, :] + in_ref[at + 16 : at + 32, :]) + (
            in_ref[at + 32 : at + 48, :] + in_ref[at + 48 : at + 64, :]
        )
        total = pltpu.roll(total, 16 - FIRST, 0)
        for core in range(2):
            out_ref[pl.ds(core * 4 + TURN[y], 16, 8), :] = total


def folded(arrived):
    return pl.pallas_call(
        fold_kernel,
        out_shape=pltpu.VMEM((128, 128), F32),
        in_specs=[VMEM],
        out_specs=VMEM,
        name="fold",
    )(near(arrived))


def line_kernel(in_ref, hi_ref, lo_ref, out_ref, turned):
    rows = [in_ref[pl.ds(y, 16, 8), :] + in_ref[pl.ds(y + 4, 16, 8), :] for y in range(4)]
    turned[...] = jnp.concatenate(rows + rows, axis=0).T
    lower = lax.broadcasted_iota(jnp.int32, (32, 128), 1) < 64
    halves = [jnp.where(lower, turned[pl.ds(2 * b, 32, 4), :], turned[pl.ds(2 * b + 1, 32, 4), :]) for b in range(2)]
    a_hi, a_lo = split_value(jnp.concatenate(halves, axis=1))
    hi = hi_ref[...]
    r = dot(a_hi, hi) + dot(a_hi, lo_ref[...]) + dot(a_lo, hi)
    first = lax.broadcasted_iota(jnp.int32, (8, N), 0) < 4
    for j in range(4):
        own = r[j * 8 : j * 8 + 8, :N]
        other = pltpu.roll(r[j * 8 : j * 8 + 8, N:], 4, 0)
        v = own + jnp.where(first, other, -other)
        for x in range(4):
            out_ref[x, j * 8 : j * 8 + 8, :] = v


def line_part(arrived, hi, lo):
    return pl.pallas_call(
        line_kernel,
        out_shape=pltpu.VMEM((4, 32, N), F32),
        in_specs=[VMEM] * 3,
        out_specs=VMEM,
        scratch_shapes=[pltpu.VMEM((128, 128), F32)],
        name="line_part",
    )(near(arrived), near(hi), near(lo))


def charge_kernel(v_ref, q_ref, wave_ref, ca_ref, sa_ref, vg_out, d_ref, mixed, vg_ref, sem):
    for s in range(16):
        top = (TURN[s // 4] * 4 + s % 4) * 8
        for c in range(4):
            vg_ref[c, 0, s : s + 1, :] = v_ref[top + c : top + c + 1, :]
            vg_ref[c, 1, s : s + 1, :] = v_ref[top + 4 + c : top + 5 + c, :]
    save = pltpu.make_async_copy(vg_ref, vg_out, sem)
    save.start()
    for s in range(16):
        top = (TURN[s // 4] * 4 + s % 4) * 8
        for a in range(0, 128, 16):
            ca = ca_ref[a : a + 16, s : s + 1]
            sa = sa_ref[a : a + 16, s : s + 1]
            cb = wave_ref[a : a + 16, :N]
            sb = wave_ref[a : a + 16, N:]
            cosine = ca * cb - sa * sb
            sine = sa * cb + ca * sb
            for c in range(4):
                real = v_ref[top + c : top + c + 1, :]
                imag = v_ref[top + 4 + c : top + 5 + c, :]
                mixed[c * 128 + a : c * 128 + a + 16, s * N : (s + 1) * N] = (real * cosine - imag * sine).astype(BF16)
    d = lax.dot_general(q_ref[...], mixed[...], (((1,), (1,)), ((), ())), preferred_element_type=F32)
    for c in range(4):
        d_ref[pl.ds(c, 171, 4), :] = d[:, c * 128 : (c + 1) * 128]
    d_ref[684:704, :] = jnp.zeros((20, 128), F32)
    save.wait()


def charge_part(v, charge, wave, ca, sa):
    return pl.pallas_call(
        charge_kernel,
        out_shape=(jax.ShapeDtypeStruct((4, 2, 16, N), F32), pltpu.VMEM((704, 128), F32)),
        in_specs=[VMEM] * 5,
        out_specs=(pl.BlockSpec(memory_space=pl.ANY), VMEM),
        scratch_shapes=[
            pltpu.VMEM((512, 4096), BF16),
            pltpu.VMEM((4, 2, 16, N), F32),
            pltpu.SemaphoreType.DMA(()),
        ],
        name="charge_part",
    )(near(v), near(charge), near(wave), near(ca), near(sa))


def meet_kernel(in_ref, out_ref, half):
    total = in_ref[0:88, :]
    for m in range(1, 8):
        total = total + in_ref[m * 88 : (m + 1) * 88, :]
    half[...] = total
    own = half[0:44, :] + half[44:88, :]
    for m in range(4):
        out_ref[m * 44 : (m + 1) * 44, :] = own


def met(arrived):
    return pl.pallas_call(
        meet_kernel,
        out_shape=pltpu.VMEM((176, 128), F32),
        in_specs=[VMEM],
        out_specs=VMEM,
        scratch_shapes=[pltpu.VMEM((88, 128), F32)],
        name="meet",
    )(near(arrived))


def total_kernel(in_ref, out_ref, half):
    half[...] = in_ref[0:88, :] + in_ref[88:176, :]
    own = half[0:44, :] + half[44:88, :]
    half[0:44, :] = own
    half[44:88, :] = own
    pair = half[...]
    for m in range(8):
        out_ref[m * 88 : (m + 1) * 88, :] = pair


def totals(arrived):
    return pl.pallas_call(
        total_kernel,
        out_shape=pltpu.VMEM((704, 128), F32),
        in_specs=[VMEM],
        out_specs=VMEM,
        scratch_shapes=[pltpu.VMEM((88, 128), F32)],
        name="totals",
    )(near(arrived))


def exchange(parts, axes, groups=None):
    return lax.all_to_all(parts, axes, split_axis=0, concat_axis=0, tiled=True, axis_index_groups=groups)


def body(potential, stick_mill, positions, aug_charge):
    (hi, lo), (line_hi, line_lo) = tables()
    hi, lo, line_hi, line_lo = map(jnp.asarray, (hi, lo, line_hi, line_lo))
    part, wave, ca, sa = plane_part(potential.reshape(16, 32, N), stick_mill, positions, hi, lo)
    arrived = exchange(part.reshape(16, 16, 128), ("y", "x"), [SQUARE])
    lines = folded(arrived.reshape(256, 128))
    arrived = exchange(lines.reshape(32, 1, 512), ("zh", "zl", "core"), [LINE])
    copies = line_part(arrived.reshape(128, 128), line_hi, line_lo)
    v = exchange(copies, "x", [TURN]).reshape(128, N)
    v, aug_charge = lax.optimization_barrier((v, aug_charge))
    charge = aug_charge.reshape(171, 16 * N)
    vg, part = charge_part(v, charge, wave, ca, sa)
    arrived = exchange(part.reshape(16, 1, 5632), FFT, NEAR)
    mid = met(arrived.reshape(704, 128))
    arrived = exchange(mid.reshape(4, 1, 5632), FFT, CROSS)
    own = totals(arrived.reshape(176, 128))
    whole = exchange(own.reshape(16, 1, 5632), FFT, NEAR)
    return vg, jnp.moveaxis(whole.reshape(176, 4, 128)[:171], 1, 0)


def solution(mesh):
    fine = Mesh(mesh.devices.reshape(4, 4, 4, 4, 2), ("y", "zh", "zl", "x", "core"))
    placed = (P(None, FFT, GRP, None), P(), P(None, GRP), P(None, FFT, None))
    return jax.shard_map(
        body,
        mesh=fine,
        in_specs=placed,
        out_specs=(P(None, None, FFT, None), P(None, None, GRP)),
        check_vma=False,
    )
```

```python
import math

import jax
import jax.numpy as jnp
import numpy as np
from jax import lax
from jax.experimental import pallas as pl
from jax.experimental.pallas import tpu as pltpu
from jax.sharding import Mesh
from jax.sharding import PartitionSpec as P

N = 256
H = 128
GRP = ("x", "core")
FFT = ("y", "zh", "zl")
F32 = jnp.float32
BF16 = jnp.bfloat16
VMEM = pl.BlockSpec(memory_space=pltpu.VMEM)

FIRST = 10
LINE = [2 * ((FIRST + i) % 16) + core for i in range(16) for core in (1, 0)]
FAR = [[2, 7, 11, 13], [0, 5, 9, 14], [1, 6, 8, 12], [3, 4, 10, 15]]
LEADS = [11, 9, 8, 10]
TURN = [2, 3, 0, 1]
SQUARE = [4 * y + x for y in TURN for x in TURN]
NEAR = [[16 * y + four[b] for four in FAR for y in TURN] for b in range(4)]
CROSS = [[16 * y + z for z in [lead] + [z for z in four if z != lead]] for four, lead in zip(FAR, LEADS) for y in range(4)]


def split_table(table):
    high = table.astype(np.float32).astype(jnp.bfloat16)
    low = (table - high.astype(np.float64)).astype(np.float32).astype(jnp.bfloat16)
    return high, low


def wave_table(left, right):
    angle = 2.0 * math.pi / N * np.mod(np.outer(left, right), N)
    return np.concatenate([np.cos(angle), np.sin(angle)], axis=1)


def tables():
    index = np.arange(N)
    flat = split_table(wave_table(index, index[:H]))
    z4, f = np.meshgrid(np.arange(4), np.arange(64), indexing="ij")
    f = f // 16 * 16 + (f + FIRST) % 16
    plane = (f * 4 + z4).reshape(-1)
    line = split_table(wave_table(plane, index - N // 2) * float(N) ** -1.5)
    return flat, line


def split_value(x):
    high = x.astype(BF16)
    return high, (x - high.astype(F32)).astype(BF16)


def dot(a, b):
    return jnp.dot(a, b, preferred_element_type=F32)


def fitted(values, degree=8):
    fit = np.polynomial.chebyshev.Chebyshev.interpolate(lambda w: values(np.sqrt(w)), degree, domain=[0.0, 1.0])
    return [float(c) for c in fit.convert(kind=np.polynomial.Polynomial).coef]


def turn_of(k):
    u = (k - H).astype(F32) * (1.0 / H)
    w = u * u
    even = fitted(lambda r: -np.cos(math.pi * r))
    odd = fitted(lambda r: -math.pi * np.sinc(r))
    cosine = jnp.full_like(u, even[-1])
    sine = jnp.full_like(u, odd[-1])
    for e, o in zip(even[-2::-1], odd[-2::-1]):
        cosine = cosine * w + e
        sine = sine * w + o
    return cosine, sine * u


def near(x):
    return pltpu.with_memory_space_constraint(x, pltpu.VMEM)


def picks(index):
    grid = lax.broadcasted_iota(jnp.int32, (H, 1024), 0)
    hit = grid == jnp.abs(index)
    even = jnp.where(hit, 1.0, 0.0).astype(BF16)
    odd = jnp.where(hit, jnp.where(index < 0, -1.0, 1.0), 0.0).astype(BF16)
    return jnp.concatenate([even, even], axis=0), jnp.concatenate([odd, odd], axis=0)


def place(axes):
    return lax.axis_index(axes)


def plane_kernel(pot_ref, mill_ref, pos_ref, hi_ref, lo_ref, out_ref, wave_ref, cos_ref, sin_ref, *scratch):
    pot, mill, pos, hi, lo, chosen, turned, sems = scratch
    loads = [
        pltpu.make_async_copy(mill_ref, mill, sems.at[0]),
        pltpu.make_async_copy(pos_ref, pos, sems.at[1]),
        pltpu.make_async_copy(hi_ref, hi, sems.at[2]),
        pltpu.make_async_copy(lo_ref, lo, sems.at[3]),
    ]
    chunks = [
        pltpu.make_async_copy(pot_ref.at[:, pl.ds(8 * q, 8), pl.ds(h * H, H)], pot.at[q, h], sems.at[4 + 2 * q + h])
        for q in range(4)
        for h in range(2)
    ]
    for load in loads + chunks:
        load.start()
    grp = place(GRP)
    fft = place(FFT)
    loads[0].wait()
    even_x, odd_x = picks(mill[0:1, :])
    even_y, odd_y = picks(mill[1:2, :])
    loads[1].wait()
    cols = jnp.concatenate([pos[...].astype(F32), jnp.zeros((125, 128), F32)], axis=0).T
    block = pl.multiple_of((fft >> 3) * 128, 128)
    shift = (128 - (fft & 7) * 16) & 127
    near_mill = jnp.concatenate([mill[:, pl.ds(block, 128)].astype(F32), jnp.zeros((6, 128), F32)], axis=0)
    mine = pltpu.roll(near_mill, shift, 1)
    k = (cols[:, 0:1] * mine[0:1, :] + cols[:, 1:2] * mine[1:2, :]).astype(jnp.int32)
    cos_ref[...], sin_ref[...] = turn_of(jnp.bitwise_and(k, N - 1))
    zcol = cols[:, 2:3].astype(jnp.int32)
    grid = lax.broadcasted_iota(jnp.int32, (128, N), 1)
    pick = jnp.where(grid == zcol, 1.0, 0.0).astype(BF16)
    sign = 1.0 - 2.0 * jnp.bitwise_and(zcol, 1).astype(F32)
    loads[2].wait()
    loads[3].wait()
    wave = dot(pick, hi[...]) + dot(pick, lo[...])
    turn = wave * sign
    wave_ref[:, 0:H] = turn[:, :H]
    wave_ref[:, H:N] = wave[:, :H]
    wave_ref[:, N : N + H] = turn[:, H:]
    wave_ref[:, N + H :] = wave[:, H:]

    start = pl.multiple_of(grp * 32, 32)
    near_hi = hi[pl.ds(start, 32), :]
    near_lo = lo[pl.ds(start, 32), :]
    cos_y = dot(jnp.concatenate([near_hi[:, :H], near_lo[:, :H]], axis=1), even_y)
    sin_y = dot(jnp.concatenate([near_hi[:, H:], near_lo[:, H:]], axis=1), odd_y)
    wide = jnp.concatenate([hi[...], lo[...], hi[...]], axis=0)
    for q in range(4):
        halves = []
        for h in range(2):
            chunks[2 * q + h].wait()
            rows = pot.at[q, h].reshape(128, H)
            halves.append(jnp.concatenate([rows[pl.ds(y, 16, 8), :] for y in range(8)], axis=0))
        x = jnp.concatenate(halves, axis=1)
        p_hi, p_lo = split_value(x)
        w_hi, w_lo = split_value(dot(jnp.concatenate([p_hi, p_hi, p_lo], axis=1), wide))
        at = q * 128
        chosen[0, at : at + 128, 0:H] = w_hi[:, :H]
        chosen[0, at : at + 128, H:N] = w_lo[:, :H]
        chosen[1, at : at + 128, 0:H] = w_hi[:, H:]
        chosen[1, at : at + 128, H:N] = w_lo[:, H:]
    for b in range(4):
        at = b * N
        even = dot(chosen[0], even_x[:, at : at + N])
        odd = dot(chosen[1], odd_x[:, at : at + N])
        real = jnp.zeros((16, N), F32)
        imag = jnp.zeros((16, N), F32)
        for y in range(32):
            e = even[y * 16 : (y + 1) * 16, :]
            o = odd[y * 16 : (y + 1) * 16, :]
            cy = cos_y[y : y + 1, at : at + N]
            sy = sin_y[y : y + 1, at : at + N]
            real = real + (e * cy - o * sy)
            imag = imag - (e * sy + o * cy)
        for h in range(2):
            part = jnp.concatenate([real[:, h * H : (h + 1) * H], imag[:, h * H : (h + 1) * H]], axis=0)
            turned[at + h * H : at + (h + 1) * H, :] = jnp.concatenate([part] * 4, axis=0).T
    lane = lax.broadcasted_iota(jnp.int32, (16, 128), 1)
    for y in range(4):
        for x in range(4):
            base = TURN[y] * 256 + TURN[x] * 4
            parts = [turned[pl.ds(base + j, 16, 16), :] for j in range(4)]
            low = jnp.where(lane < 32, parts[0], parts[1])
            high = jnp.where(lane < 96, parts[2], parts[3])
            at = (y * 4 + x) * 16
            out_ref[at : at + 16, :] = jnp.where(lane < 64, low, high)


def plane_part(potential, stick_mill, positions, hi, lo):
    return pl.pallas_call(
        plane_kernel,
        out_shape=(
            pltpu.VMEM((256, 128), F32),
            pltpu.VMEM((128, 2 * N), F32),
            pltpu.VMEM((128, 128), F32),
            pltpu.VMEM((128, 128), F32),
        ),
        in_specs=[pl.BlockSpec(memory_space=pl.ANY)] * 5,
        out_specs=(VMEM,) * 4,
        scratch_shapes=[
            pltpu.VMEM((4, 2, 16, 8, H), F32),
            pltpu.VMEM((2, 1024), jnp.int32),
            pltpu.VMEM((3, 128), jnp.int32),
            pltpu.VMEM((N, N), BF16),
            pltpu.VMEM((N, N), BF16),
            pltpu.VMEM((2, 512, N), BF16),
            pltpu.VMEM((1024, 128), F32),
            pltpu.SemaphoreType.DMA((12,)),
        ],
        name="plane_part",
    )(potential, stick_mill, positions, hi, lo)


def fold_kernel(in_ref, out_ref):
    for y in range(4):
        at = y * 64
        total = (in_ref[at : at + 16, :] + in_ref[at + 16 : at + 32, :]) + (
            in_ref[at + 32 : at + 48, :] + in_ref[at + 48 : at + 64, :]
        )
        total = pltpu.roll(total, 16 - FIRST, 0)
        for core in range(2):
            out_ref[pl.ds(core * 4 + TURN[y], 16, 8), :] = total


def folded(arrived):
    return pl.pallas_call(
        fold_kernel,
        out_shape=pltpu.VMEM((128, 128), F32),
        in_specs=[VMEM],
        out_specs=VMEM,
        name="fold",
    )(near(arrived))


def line_kernel(in_ref, hi_ref, lo_ref, out_ref, turned):
    rows = [in_ref[pl.ds(y, 16, 8), :] + in_ref[pl.ds(y + 4, 16, 8), :] for y in range(4)]
    turned[...] = jnp.concatenate(rows + rows, axis=0).T
    lower = lax.broadcasted_iota(jnp.int32, (32, 128), 1) < 64
    halves = [jnp.where(lower, turned[pl.ds(2 * b, 32, 4), :], turned[pl.ds(2 * b + 1, 32, 4), :]) for b in range(2)]
    a_hi, a_lo = split_value(jnp.concatenate(halves, axis=1))
    hi = hi_ref[...]
    r = dot(a_hi, hi) + dot(a_hi, lo_ref[...]) + dot(a_lo, hi)
    first = lax.broadcasted_iota(jnp.int32, (8, N), 0) < 4
    for j in range(4):
        own = r[j * 8 : j * 8 + 8, :N]
        other = pltpu.roll(r[j * 8 : j * 8 + 8, N:], 4, 0)
        v = own + jnp.where(first, other, -other)
        for x in range(4):
            out_ref[x, j * 8 : j * 8 + 8, :] = v


def line_part(arrived, hi, lo):
    return pl.pallas_call(
        line_kernel,
        out_shape=pltpu.VMEM((4, 32, N), F32),
        in_specs=[VMEM] * 3,
        out_specs=VMEM,
        scratch_shapes=[pltpu.VMEM((128, 128), F32)],
        name="line_part",
    )(near(arrived), near(hi), near(lo))


def charge_kernel(v_ref, q_ref, wave_ref, ca_ref, sa_ref, vg_out, d_ref, mixed, vg_ref, sem):
    for s in range(16):
        top = (TURN[s // 4] * 4 + s % 4) * 8
        for c in range(4):
            vg_ref[c, 0, s : s + 1, :] = v_ref[top + c : top + c + 1, :]
            vg_ref[c, 1, s : s + 1, :] = v_ref[top + 4 + c : top + 5 + c, :]
    save = pltpu.make_async_copy(vg_ref, vg_out, sem)
    save.start()
    for s in range(16):
        top = (TURN[s // 4] * 4 + s % 4) * 8
        for a in range(0, 128, 16):
            ca = ca_ref[a : a + 16, s : s + 1]
            sa = sa_ref[a : a + 16, s : s + 1]
            cb = wave_ref[a : a + 16, :N]
            sb = wave_ref[a : a + 16, N:]
            cosine = ca * cb - sa * sb
            sine = sa * cb + ca * sb
            for c in range(4):
                real = v_ref[top + c : top + c + 1, :]
                imag = v_ref[top + 4 + c : top + 5 + c, :]
                mixed[c * 128 + a : c * 128 + a + 16, s * N : (s + 1) * N] = (real * cosine - imag * sine).astype(BF16)
    d = lax.dot_general(q_ref[...], mixed[...], (((1,), (1,)), ((), ())), preferred_element_type=F32)
    for c in range(4):
        d_ref[pl.ds(c, 171, 4), :] = d[:, c * 128 : (c + 1) * 128]
    d_ref[684:704, :] = jnp.zeros((20, 128), F32)
    save.wait()


def charge_part(v, charge, wave, ca, sa):
    return pl.pallas_call(
        charge_kernel,
        out_shape=(jax.ShapeDtypeStruct((4, 2, 16, N), F32), pltpu.VMEM((704, 128), F32)),
        in_specs=[VMEM] * 5,
        out_specs=(pl.BlockSpec(memory_space=pl.ANY), VMEM),
        scratch_shapes=[
            pltpu.VMEM((512, 4096), BF16),
            pltpu.VMEM((4, 2, 16, N), F32),
            pltpu.SemaphoreType.DMA(()),
        ],
        name="charge_part",
    )(near(v), near(charge), near(wave), near(ca), near(sa))


def meet_kernel(in_ref, out_ref, half):
    total = in_ref[0:88, :]
    for m in range(1, 8):
        total = total + in_ref[m * 88 : (m + 1) * 88, :]
    half[...] = total
    own = half[0:44, :] + half[44:88, :]
    for m in range(4):
        out_ref[m * 44 : (m + 1) * 44, :] = own


def met(arrived):
    return pl.pallas_call(
        meet_kernel,
        out_shape=pltpu.VMEM((176, 128), F32),
        in_specs=[VMEM],
        out_specs=VMEM,
        scratch_shapes=[pltpu.VMEM((88, 128), F32)],
        name="meet",
    )(near(arrived))


def total_kernel(in_ref, out_ref, half):
    half[...] = in_ref[0:88, :] + in_ref[88:176, :]
    own = half[0:44, :] + half[44:88, :]
    half[0:44, :] = own
    half[44:88, :] = own
    pair = half[...]
    for m in range(8):
        out_ref[m * 88 : (m + 1) * 88, :] = pair


def totals(arrived):
    return pl.pallas_call(
        total_kernel,
        out_shape=pltpu.VMEM((704, 128), F32),
        in_specs=[VMEM],
        out_specs=VMEM,
        scratch_shapes=[pltpu.VMEM((88, 128), F32)],
        name="totals",
    )(near(arrived))


def exchange(parts, axes, groups=None):
    return lax.all_to_all(parts, axes, split_axis=0, concat_axis=0, tiled=True, axis_index_groups=groups)


def body(potential, stick_mill, positions, aug_charge):
    (hi, lo), (line_hi, line_lo) = tables()
    hi, lo, line_hi, line_lo = map(jnp.asarray, (hi, lo, line_hi, line_lo))
    part, wave, ca, sa = plane_part(potential.reshape(16, 32, N), stick_mill, positions, hi, lo)
    arrived = exchange(part.reshape(16, 16, 128), ("y", "x"), [SQUARE])
    lines = folded(arrived.reshape(256, 128))
    arrived = exchange(lines.reshape(32, 1, 512), ("zh", "zl", "core"), [LINE])
    copies = line_part(arrived.reshape(128, 128), line_hi, line_lo)
    v = exchange(copies, "x", [TURN]).reshape(128, N)
    v, aug_charge = lax.optimization_barrier((v, aug_charge))
    charge = aug_charge.reshape(171, 16 * N)
    vg, part = charge_part(v, charge, wave, ca, sa)
    arrived = exchange(part.reshape(16, 1, 5632), FFT, NEAR)
    mid = met(arrived.reshape(704, 128))
    arrived = exchange(mid.reshape(4, 1, 5632), FFT, CROSS)
    own = totals(arrived.reshape(176, 128))
    whole = exchange(own.reshape(16, 1, 5632), FFT, NEAR)
    return vg, jnp.moveaxis(whole.reshape(176, 4, 128)[:171], 1, 0)


def solution(mesh):
    fine = Mesh(mesh.devices.reshape(4, 4, 4, 4, 2), ("y", "zh", "zl", "x", "core"))
    placed = (P(None, FFT, GRP, None), P(), P(None, GRP), P(None, FFT, None))
    return jax.shard_map(
        body,
        mesh=fine,
        in_specs=placed,
        out_specs=(P(None, None, FFT, None), P(None, None, GRP)),
        check_vma=False,
    )
```
